128 devices in a mesh: px: 8 (over z_lo, y), py: 16 (over x, z_hi, core).
Axes of the slice: x: 4, y: 4, z: 4 (z_hi: 2, z_lo: 2; z = z_hi * 2 + z_lo), core: 2. Of those that a mesh axis runs over, the one named last changes fastest.
Arguments:
- field: bfloat16 [32, 128, 128, 128], P(None, 'px', 'py'), may hold values from -6 to 6
- spec_fine: bfloat16 [2, 32, 32, 32, 32, 32], P(None, None, None, None, 'px', 'py'), may hold values from -18 to 18
- mix_fine: bfloat16 [32, 32], replicated, may hold values from -1 to 1
- bias_fine: float32 [32], replicated, may hold values from -3 to 3
- spec_coarse: bfloat16 [2, 32, 32, 32, 32, 32], P(None, None, None, None, 'px', 'py'), may hold values from -12 to 12
- mix_coarse: bfloat16 [32, 32], replicated, may hold values from -1 to 1
- bias_coarse: float32 [32], replicated, may hold values from -3 to 3
Outputs:
- output: bfloat16 [32, 128, 128, 128], P(None, 'px', 'py')
The draws below stay inside these ranges and needn't reach their ends.
All inputs are finite; a program needn't handle non-finite values.
Results may differ from the reference program's by a relative error of at most 0.0085.
Values may be sent and summed in bfloat16 or wider, within the bound.
No kernel may reach another device: no remote copies, remote signals or barrier semaphores. Data moves between devices by JAX's collectives and lax.ppermute only.
A program may use at most 128 MiB of HBM per device.

```python
import math
import jax
import jax.numpy as jnp
from jax import lax

C = 32
N = 128
KX = 32
KY = 32
KZ = 32


def level_of(rng, shape, split, smallest, largest):
    gain = 1.0
    for position, shards_of in split:
        heights = jax.random.uniform(jax.random.fold_in(jax.random.fold_in(rng, 6), position), (shards_of,), jnp.float32, smallest / len(split), largest / len(split))
        gain = gain * jnp.repeat(jnp.exp(heights), shape[position] // shards_of).reshape((-1,) + (1,) * (len(shape) - 1 - position))
    return gain


def normal_values(rng, extent, spread, reach, cuts=(), kind=jnp.bfloat16):
    result = jax.random.normal(rng, extent, jnp.float32) * spread
    if len(cuts) > 0:
        result = level_of(rng, extent, cuts, -0.22, 0.18) * result
    return jnp.clip(result, min=-reach, max=reach).astype(kind)


def setup_inputs(seed: int = 0) -> dict:
    streams_of = jax.random.split(jax.random.key(seed), 8)
    return {
        "field": normal_values(streams_of[0], (C, N, N, N), 1.0, 6.0, ((1, 8), (2, 16))),
        "spec_fine": normal_values(streams_of[1], (2, C, C, KX, KY, KZ), 3.0, 18.0, ((4, 8), (5, 16))),
        "mix_fine": normal_values(streams_of[2], (C, C), C ** -0.5, 1.0),
        "bias_fine": normal_values(streams_of[3], (C,), 0.5, 3.0, (), jnp.float32),
        "spec_coarse": normal_values(streams_of[4], (2, C, C, KX, KY, KZ), 2.0, 12.0, ((4, 8), (5, 16))),
        "mix_coarse": normal_values(streams_of[5], (C, C), C ** -0.5, 1.0),
        "bias_coarse": normal_values(streams_of[6], (C,), 0.5, 3.0, (), jnp.float32),
    }


highest = lax.Precision.HIGHEST


def phases(cells, modes, offset):
    places = jnp.arange(cells, dtype=jnp.int32)
    frequency = jnp.arange(modes, dtype=jnp.int32) - offset
    windings = (places[:, None] * frequency[None, :]) % cells
    return windings.astype(jnp.float32) * (2.0 * math.pi / cells)


def forward_table(cells, modes, offset):
    angle = phases(cells, modes, offset)
    return jnp.stack([jnp.cos(angle), -jnp.sin(angle)]).astype(jnp.bfloat16)


def inverse_table(cells, modes, offset):
    angle = phases(cells, modes, offset)
    return jnp.transpose(jnp.stack([jnp.cos(angle), jnp.sin(angle)]), (0, 2, 1))


def depth_inverse(cells, modes):
    angle = phases(cells, modes, 0)
    factor = jnp.where(jnp.arange(modes) == 0, 1.0, 2.0).astype(jnp.float32) / float(cells * cells * cells)
    return jnp.transpose(jnp.stack([factor[None, :] * jnp.cos(angle), -factor[None, :] * jnp.sin(angle)]), (0, 2, 1))


def complex_dot(data, table, form):
    real = jnp.einsum(form, data[0], table[0], precision=highest) - jnp.einsum(form, data[1], table[1], precision=highest)
    imag = jnp.einsum(form, data[0], table[1], precision=highest) + jnp.einsum(form, data[1], table[0], precision=highest)
    return jnp.stack([real, imag])


def mix_modes(modes, spectral):
    weights = spectral.astype(jnp.float32)
    form = "ijmk,iojmk->ojmk"
    real = jnp.einsum(form, modes[0], weights[0], precision=highest) - jnp.einsum(form, modes[1], weights[1], precision=highest)
    imag = jnp.einsum(form, modes[0], weights[1], precision=highest) + jnp.einsum(form, modes[1], weights[0], precision=highest)
    return jnp.stack([real, imag])


def spectral_layer(field, spectral, mixing, offsets):
    channels, cells = field.shape[0], field.shape[1]
    row_block = 16 if cells % 16 == 0 else cells
    depth_table = forward_table(cells, KZ, 0).astype(jnp.float32)
    column_table = forward_table(cells, KY, KY // 2).astype(jnp.float32)
    row_table = forward_table(cells, KX, KX // 2).astype(jnp.float32)

    def gather_step(total, slab_index):
        slab = lax.dynamic_slice_in_dim(field, slab_index * row_block, row_block, 1).astype(jnp.float32)
        depth = jnp.einsum("cxyz,rzk->rcxyk", slab, depth_table, precision=highest)
        across = complex_dot(depth, column_table, "cxyk,ym->cxmk")
        part_table = lax.dynamic_slice_in_dim(row_table, slab_index * row_block, row_block, 1)
        return total + complex_dot(across, part_table, "cxmk,xj->cjmk"), None

    start_modes = jnp.zeros((2, channels, KX, KY, KZ), jnp.float32)
    modes, _ = lax.scan(gather_step, start_modes, jnp.arange(cells // row_block, dtype=jnp.int32))
    mixed = mix_modes(modes, spectral)
    row_inverse = inverse_table(cells, KX, KX // 2)
    column_inverse = inverse_table(cells, KY, KY // 2)
    depth_back = depth_inverse(cells, KZ)
    mixing_wide = mixing.astype(jnp.float32)

    def slab_out(slab_index):
        part_table = lax.dynamic_slice_in_dim(row_inverse, slab_index * row_block, row_block, 2)
        rows_back = complex_dot(mixed, part_table, "cjmk,jx->cxmk")
        columns_back = complex_dot(rows_back, column_inverse, "cxmk,my->cxyk")
        spectral_part = jnp.einsum("cxyk,kz->cxyz", columns_back[0], depth_back[0], precision=highest)
        spectral_part = spectral_part + jnp.einsum("cxyk,kz->cxyz", columns_back[1], depth_back[1], precision=highest)
        slab = lax.dynamic_slice_in_dim(field, slab_index * row_block, row_block, 1).astype(jnp.float32)
        pointwise = jnp.einsum("cxyz,co->oxyz", slab, mixing_wide, precision=highest)
        total = spectral_part + pointwise + offsets[:, None, None, None].astype(jnp.float32)
        return jax.nn.gelu(total).astype(jnp.bfloat16)

    blocks = lax.map(slab_out, jnp.arange(cells // row_block, dtype=jnp.int32))
    return jnp.transpose(blocks, (1, 0, 2, 3, 4)).reshape(channels, cells, cells, cells)


def reference(field, spec_fine, mix_fine, bias_fine, spec_coarse, mix_coarse, bias_coarse):
    upper = spectral_layer(field, spec_fine, mix_fine, bias_fine)
    channels, rows_x, rows_y, cells = upper.shape
    blocks = upper.astype(jnp.float32).reshape(channels, rows_x // 2, 2, rows_y // 2, 2, cells // 2, 2)
    pooled = blocks.mean(axis=(2, 4, 6)).astype(jnp.bfloat16)
    lower = spectral_layer(pooled, spec_coarse, mix_coarse, bias_coarse)
    merged = blocks + lower.astype(jnp.float32)[:, :, None, :, None, :, None]
    return merged.reshape(channels, rows_x, rows_y, cells).astype(jnp.bfloat16)
```

```python
import functools
import math

import jax
import jax.numpy as jnp
import numpy as np
from jax import lax
from jax.experimental import pallas as pl
from jax.experimental.pallas import tpu as pltpu
from jax.sharding import PartitionSpec as P

C = 32
KEPT = 32
F32 = jnp.float32
BF16 = jnp.bfloat16


def angles(cells, offset):
    windings = np.arange(cells)[:, None] * (np.arange(KEPT)[None, :] - offset) % cells
    return windings.astype(np.float64) * (2.0 * math.pi / cells)


def depth_forward(cells, repeat):
    angle = angles(cells, 0)
    table = np.stack([np.cos(angle), -np.sin(angle)])
    table = table.reshape(2, cells, 16, 2).transpose(1, 2, 0, 3)
    spread = np.zeros((cells, repeat) + table.shape[1:])
    spread[:, 0] = table
    spread = spread.reshape((cells * repeat,) + table.shape[1:])
    result = np.einsum("zprk,hg->hzprkg", spread, np.eye(4))
    return result.reshape(4 * cells * repeat, 256).astype(BF16)


def plane_forward(cells):
    angle = angles(cells, KEPT // 2)
    return np.concatenate([np.cos(angle), -np.sin(angle)], axis=1).T.astype(BF16)


def halves(table):
    high = table.astype(np.float32).astype(BF16)
    low = (table.astype(np.float32) - high.astype(np.float32)).astype(BF16)
    return high, low


def plane_inverse(cells):
    angle = angles(cells, KEPT // 2)
    high, low = halves(np.concatenate([np.cos(angle), np.sin(angle)], axis=1))
    return np.concatenate([high, low], axis=1)


def depth_inverse(cells, repeat):
    angle = angles(cells, 0)
    factor = np.where(np.arange(KEPT) == 0, 1.0, 2.0) / float(cells**3)
    table = np.stack([factor * np.cos(angle), -factor * np.sin(angle)])
    table = np.repeat(table, repeat, axis=1).reshape(2, cells * repeat, 16, 2)
    result = np.einsum("rzpk,hg->prkhgz", table, np.eye(4)).reshape(256, 4 * cells * repeat)
    return np.concatenate(halves(result), axis=0)


def dot(a, b):
    return jnp.dot(a, b, preferred_element_type=F32)


def lanes_of(shape):
    return lax.broadcasted_iota(jnp.int32, shape, len(shape) - 1)


def turn(x):
    width = x.shape[-1]
    real = (lanes_of(x.shape) & 8) == 0
    return jnp.where(real, -pltpu.roll(x, width - 8, 1), pltpu.roll(x, 8, 1))


def swap_blocks(parts):
    parts = list(parts)
    lane = lanes_of(parts[0].shape)
    for step in (1, 2, 4):
        keep = (lane & (16 * step)) == 0
        for low in range(8):
            if low & step == 0:
                a, b = parts[low], parts[low + step]
                parts[low] = jnp.where(keep, a, pltpu.roll(b, 16 * step, 1))
                parts[low + step] = jnp.where(keep, pltpu.roll(a, 128 - 16 * step, 1), b)
    return parts


def spread_groups(product, send, rows):
    def chunk(index, carry):
        at = pl.ds(pl.multiple_of(index * 16, 16), 16)
        for half in range(2):
            parts = swap_blocks([product[g, at, 128 * half : 128 * half + 128] for g in range(8)])
            for b in range(8):
                send[8 * half + b, at, :] = parts[b].astype(BF16)
        return carry

    lax.fori_loop(0, rows // 16, chunk, 0)


def collect_groups(received, spread, rows):
    def chunk(index, carry):
        at = pl.ds(pl.multiple_of(index * 16, 16), 16)
        for half in range(2):
            parts = swap_blocks([received[8 * half + b, at, :].astype(F32) for b in range(8)])
            for g in range(8):
                spread[g, at, 128 * half : 128 * half + 128] = parts[g].astype(BF16)
        return carry

    lax.fori_loop(0, rows // 16, chunk, 0)


def depth_kernel(field, table, send, product):
    for g in range(8):
        rows = jnp.concatenate([field[8 * h + g] for h in range(4)], axis=1)
        product[g] = dot(rows, table[...])
    spread_groups(product, send, 128)


def columns_fine_kernel(received, table, send, lines):
    for pair in range(8):
        block = received[:, 16 * pair : 16 * pair + 16, :].astype(F32).reshape(16, 2, 8, 128)
        data = jnp.concatenate([block[:, e].reshape(128, 128) for e in range(2)], axis=1)
        out = dot(table[...], data.astype(BF16))
        out = out[:KEPT] + turn(out[KEPT:])
        for e in range(2):
            lines[pl.ds(2 * pair + e, KEPT, stride=16), :] = out[:, 128 * e : 128 * e + 128]
    send[...] = lines[...].reshape(8, 64, 128).astype(BF16)


def columns_coarse_kernel(received, table, send, cells, lines):
    cells[...] = received[...].astype(F32).reshape(512, 128)
    data = jnp.concatenate([cells[pl.ds(x, 64, stride=8), :] for x in range(8)], axis=1)
    out = dot(table[...], data.astype(BF16))
    out = out[:KEPT] + turn(out[KEPT:])
    for x in range(8):
        lines[pl.ds(x, KEPT, stride=8), :] = out[:, 128 * x : 128 * x + 128]
    send[...] = lines[...].reshape(8, 32, 128).astype(BF16)


def mix_kernel(received, forward, inverse, weights, send, modes, mixed):
    own = received.shape[2]
    data = received[...].astype(F32)
    data = jnp.concatenate([data[:, m].reshape(8 * own, 128) for m in range(4)], axis=1)
    out = dot(forward[...], data.astype(BF16))
    out = out[:KEPT] + turn(out[KEPT:])
    out = jnp.concatenate([out[:, 128 * m : 128 * m + 128] for m in range(4)], axis=0)
    modes[...] = out.T

    def step(g, sums):
        sums = list(sums)
        base = g * 16
        for h in range(4):
            for k in range(2):
                real = modes[pl.ds(base + 4 * k + h, 1), :]
                imag = modes[pl.ds(base + 8 + 4 * k + h, 1), :]
                w_real = weights[0, 8 * h + g, k].astype(F32)
                w_imag = weights[1, 8 * h + g, k].astype(F32)
                sums[2 * k] = sums[2 * k] + (w_real * real - w_imag * imag)
                sums[2 * k + 1] = sums[2 * k + 1] + (w_real * imag + w_imag * real)
        return tuple(sums)

    sums = lax.fori_loop(0, 8, step, tuple(jnp.zeros((C, 128), F32) for _ in range(4)))
    for k in range(2):
        for r in range(2):
            for h in range(4):
                mixed[pl.ds(8 * r + 4 * k + h, 8, stride=16), :] = sums[2 * k + r][8 * h : 8 * h + 8]
    back = mixed[...].T
    back = jnp.concatenate([back[32 * m : 32 * m + 32] for m in range(4)], axis=1)
    back = jnp.concatenate([back, turn(back)], axis=0).astype(BF16)
    out = dot(inverse[...], jnp.concatenate([back, back], axis=0))
    for m in range(4):
        send[:, m] = out[:, 128 * m : 128 * m + 128].reshape(8, own, 128).astype(BF16)


def back_columns(lines, table, own, first, count):
    data = jnp.concatenate([lines[pl.ds(first + x, KEPT, stride=own), :] for x in range(count)], axis=1)
    data = jnp.concatenate([data, turn(data)], axis=0).astype(BF16)
    return dot(table, jnp.concatenate([data, data], axis=0))


def back_fine_kernel(received, table, send, lines):
    lines[...] = received[...].astype(F32).reshape(512, 128)
    for pair in range(8):
        out = back_columns(lines, table[...], 16, 2 * pair, 2)
        parts = [out[:, 128 * e : 128 * e + 128].reshape(16, 1, 8, 128) for e in range(2)]
        block = jnp.concatenate(parts, axis=1).reshape(16, 16, 128)
        send[:, 16 * pair : 16 * pair + 16, :] = block.astype(BF16)


def back_coarse_kernel(received, table, send, lines, cells):
    lines[...] = received[...].astype(F32).reshape(256, 128)
    out = back_columns(lines, table[...], 8, 0, 8)
    for x in range(8):
        cells[pl.ds(x, 64, stride=8), :] = out[:, 128 * x : 128 * x + 128]
    send[...] = cells[...].reshape(16, 32, 128).astype(BF16)


def channel_map(mixing):
    row = lax.broadcasted_iota(jnp.int32, (512, C), 0)
    channel = lax.broadcasted_iota(jnp.int32, (512, C), 1)
    pick = jnp.where((row >> 4) == channel, 1.0, 0.0).astype(BF16)
    wide = lax.dot_general(pick, mixing, (((1,), (1,)), ((), ())), preferred_element_type=F32)
    wide = lax.dot_general(wide.astype(BF16), pick, (((1,), (1,)), ((), ())), preferred_element_type=F32)
    a = lax.broadcasted_iota(jnp.int32, (512, 512), 0)
    b = lax.broadcasted_iota(jnp.int32, (512, 512), 1)
    return jnp.where(((a ^ b) & 15) == 0, wide, 0.0).astype(BF16)


def pointwise(values, mixing, total, rows):
    blocks = [values[:, 16 * p : 16 * p + 16, :].reshape(512, 128) for p in range(rows // 16)]
    out = dot(channel_map(mixing), jnp.concatenate(blocks, axis=1))
    for p in range(rows // 16):
        total[:, 16 * p : 16 * p + 16, :] = out[:, 128 * p : 128 * p + 128].reshape(C, 16, 128)


def gelu(v):
    inner = v * (0.7978845608028654 + 0.03567740813636141 * (v * v))
    half = 0.5 * v
    return half + half * jnp.tanh(inner)


def upper_kernel(received, table, field, mixing, bias, next_table, upper, pooled, send, spread, total, sums, product):
    pointwise(field, mixing[...], total, 128)
    collect_groups(received, spread, 128)
    even = (lanes_of((64, 128)) & 1) == 0

    def group(g, carry):
        data = spread[g]
        out = dot(jnp.concatenate([data, data], axis=1), table[...])
        for h in range(4):
            o = 8 * h + g
            value = gelu(out[:, 128 * h : 128 * h + 128] + total[o] + bias[o]).astype(BF16)
            upper[o] = value
            value = value.astype(F32).reshape(8, 2, 8, 128)
            value = (value[:, 0] + value[:, 1]).reshape(64, 128)
            value = value + jnp.where(even, pltpu.roll(value, 127, 1), pltpu.roll(value, 1, 1))
            sums[...] = value
            parts = [sums[pl.ds(2 * y, 8, stride=8), :] + sums[pl.ds(2 * y + 1, 8, stride=8), :] for y in range(4)]
            pooled[o] = (jnp.concatenate(parts, axis=0) * 0.125).astype(BF16)
        rows = jnp.concatenate([pooled[8 * h + g] for h in range(4)], axis=1)
        product[g] = dot(rows, next_table[...])
        return carry

    lax.fori_loop(0, 8, group, 0)
    spread_groups(product, send, 32)


def lower_kernel(received, table, pooled, mixing, bias, upper, out_ref, spread, total, sums):
    pointwise(pooled, mixing[...], total, 32)
    collect_groups(received, spread, 32)

    def group(g, carry):
        data = spread[g]
        out = dot(jnp.concatenate([data, data], axis=1), table[...])
        for h in range(4):
            o = 8 * h + g
            value = gelu(out[:, 128 * h : 128 * h + 128] + total[o] + bias[o]).astype(BF16).astype(F32)
            for y in range(4):
                part = value[8 * y : 8 * y + 8]
                sums[pl.ds(2 * y, 8, stride=8), :] = part
                sums[pl.ds(2 * y + 1, 8, stride=8), :] = part
            added = sums[...].reshape(8, 1, 8, 128)
            fine = upper[o].astype(F32).reshape(8, 2, 8, 128)
            out_ref[o] = (fine + added).reshape(128, 128).astype(BF16)
        return carry

    lax.fori_loop(0, 8, group, 0)


def call(kernel, outs, *operands, scratch=(), scalars=()):
    vmem = pl.BlockSpec(memory_space=pltpu.VMEM)
    smem = pl.BlockSpec(memory_space=pltpu.SMEM)
    shapes = [jax.ShapeDtypeStruct(shape, BF16) for shape in outs]
    return pl.pallas_call(
        kernel,
        out_shape=shapes if len(shapes) > 1 else shapes[0],
        in_specs=[smem if i in scalars else vmem for i in range(len(operands))],
        out_specs=[vmem] * len(shapes) if len(shapes) > 1 else vmem,
        scratch_shapes=[pltpu.VMEM(shape, kind) for shape, kind in scratch],
        compiler_params=pltpu.CompilerParams(vmem_limit_bytes=48 << 20),
    )(*operands)


def exchange(x, axis):
    return lax.all_to_all(x, axis, 0, 0, tiled=True)


def lay_out(spectral):
    turned = jnp.transpose(spectral, (0, 1, 5, 2, 4, 3))
    return jnp.concatenate([turned[..., m, :] for m in range(4)], axis=-1)


def on_device(field, spec_fine, mix_fine, bias_fine, spec_coarse, mix_coarse, bias_coarse):
    field = field.reshape(C, 128, 128)
    forward_fine, inverse_fine = jnp.asarray(plane_forward(128)), jnp.asarray(plane_inverse(128))
    forward_coarse, inverse_coarse = jnp.asarray(plane_forward(64)), jnp.asarray(plane_inverse(64))
    weights_fine = lay_out(spec_fine)
    weights_coarse = lay_out(spec_coarse)

    x = call(depth_kernel, [(16, 128, 128)], field, jnp.asarray(depth_forward(128, 1)), scratch=[((8, 128, 256), F32)])
    x = exchange(x, "py")
    x = call(columns_fine_kernel, [(8, 64, 128)], x, forward_fine, scratch=[((512, 128), F32)])
    x = exchange(x, "px").reshape(8, 4, 16, 128)
    mix_scratch = [((128, 128), F32), ((128, 128), F32)]
    x = call(mix_kernel, [(8, 4, 16, 128)], x, forward_fine, inverse_fine, weights_fine, scratch=mix_scratch)
    x = exchange(x.reshape(8, 64, 128), "px")
    x = call(back_fine_kernel, [(16, 128, 128)], x, inverse_fine, scratch=[((512, 128), F32)])
    x = exchange(x, "py")
    upper, pooled, x = call(
        upper_kernel,
        [(C, 128, 128), (C, 32, 128), (16, 32, 128)],
        x,
        jnp.asarray(depth_inverse(128, 1)),
        field,
        mix_fine,
        bias_fine,
        jnp.asarray(depth_forward(64, 2)),
        scratch=[((8, 128, 256), BF16), ((C, 128, 128), F32), ((64, 128), F32), ((8, 32, 256), F32)],
        scalars=(4,),
    )
    x = exchange(x, "py")
    x = call(columns_coarse_kernel, [(8, 32, 128)], x, forward_coarse, scratch=[((512, 128), F32), ((256, 128), F32)])
    x = exchange(x, "px").reshape(8, 4, 8, 128)
    x = call(mix_kernel, [(8, 4, 8, 128)], x, forward_coarse, inverse_coarse, weights_coarse, scratch=mix_scratch)
    x = exchange(x.reshape(8, 32, 128), "px")
    x = call(back_coarse_kernel, [(16, 32, 128)], x, inverse_coarse, scratch=[((256, 128), F32), ((512, 128), F32)])
    x = exchange(x, "py")
    out = call(
        lower_kernel,
        [(C, 128, 128)],
        x,
        jnp.asarray(depth_inverse(64, 2)),
        pooled,
        mix_coarse,
        bias_coarse,
        upper,
        scratch=[((8, 32, 256), BF16), ((C, 32, 128), F32), ((64, 128), F32)],
        scalars=(4,),
    )
    return out.reshape(C, 16, 8, 128)


def solution(mesh):
    return jax.shard_map(
        on_device,
        mesh=mesh,
        in_specs=(
            P(None, "px", "py", None),
            P(None, None, None, None, "px", "py"),
            P(),
            P(),
            P(None, None, None, None, "px", "py"),
            P(),
            P(),
        ),
        out_specs=P(None, "px", "py", None),
        check_vma=False,
    )
```

```python
import functools
import math

import jax
import jax.numpy as jnp
import numpy as np
from jax import lax
from jax.experimental import pallas as pl
from jax.experimental.pallas import tpu as pltpu
from jax.sharding import PartitionSpec as P

C = 32
KEPT = 32
F32 = jnp.float32
BF16 = jnp.bfloat16


def angles(cells, offset):
    windings = np.arange(cells)[:, None] * (np.arange(KEPT)[None, :] - offset) % cells
    return windings.astype(np.float64) * (2.0 * math.pi / cells)


def depth_forward(cells, repeat):
    angle = angles(cells, 0)
    table = np.stack([np.cos(angle), -np.sin(angle)])
    table = table.reshape(2, cells, 16, 2).transpose(1, 2, 0, 3)
    spread = np.zeros((cells, repeat) + table.shape[1:])
    spread[:, 0] = table
    spread = spread.reshape((cells * repeat,) + table.shape[1:])
    result = np.einsum("zprk,hg->hzprkg", spread, np.eye(4))
    return result.reshape(4 * cells * repeat, 256).astype(BF16)


def plane_forward(cells):
    angle = angles(cells, KEPT // 2)
    return np.concatenate([np.cos(angle), -np.sin(angle)], axis=1).T.astype(BF16)


def halves(table):
    high = table.astype(np.float32).astype(BF16)
    low = (table.astype(np.float32) - high.astype(np.float32)).astype(BF16)
    return high, low


def plane_inverse(cells):
    angle = angles(cells, KEPT // 2)
    high, low = halves(np.concatenate([np.cos(angle), np.sin(angle)], axis=1))
    return np.concatenate([high, low], axis=1)


def depth_inverse(cells, repeat):
    angle = angles(cells, 0)
    factor = np.where(np.arange(KEPT) == 0, 1.0, 2.0) / float(cells**3)
    table = np.stack([factor * np.cos(angle), -factor * np.sin(angle)])
    table = np.repeat(table, repeat, axis=1).reshape(2, cells * repeat, 16, 2)
    result = np.einsum("rzpk,hg->prkhgz", table, np.eye(4)).reshape(256, 4 * cells * repeat)
    return result.astype(BF16)


def dot(a, b):
    return jnp.dot(a, b, preferred_element_type=F32)


def lanes_of(shape):
    return lax.broadcasted_iota(jnp.int32, shape, len(shape) - 1)


def turn(x):
    width = x.shape[-1]
    real = (lanes_of(x.shape) & 8) == 0
    return jnp.where(real, -pltpu.roll(x, width - 8, 1), pltpu.roll(x, 8, 1))


def swap_blocks(parts):
    parts = list(parts)
    lane = lanes_of(parts[0].shape)
    for step in (1, 2, 4):
        keep = (lane & (16 * step)) == 0
        for low in range(8):
            if low & step == 0:
                a, b = parts[low], parts[low + step]
                parts[low] = jnp.where(keep, a, pltpu.roll(b, 16 * step, 1))
                parts[low + step] = jnp.where(keep, pltpu.roll(a, 128 - 16 * step, 1), b)
    return parts


def spread_groups(product, send, rows):
    def chunk(index, carry):
        at = pl.ds(pl.multiple_of(index * 16, 16), 16)
        for half in range(2):
            parts = swap_blocks([product[g, at, 128 * half : 128 * half + 128] for g in range(8)])
            for b in range(8):
                send[8 * half + b, at, :] = parts[b].astype(BF16)
        return carry

    lax.fori_loop(0, rows // 16, chunk, 0)


def collect_groups(received, spread, rows):
    def chunk(index, carry):
        at = pl.ds(pl.multiple_of(index * 16, 16), 16)
        for half in range(2):
            parts = swap_blocks([received[8 * half + b, at, :].astype(F32) for b in range(8)])
            for g in range(8):
                spread[g, at, 128 * half : 128 * half + 128] = parts[g].astype(BF16)
        return carry

    lax.fori_loop(0, rows // 16, chunk, 0)


def depth_kernel(field, table_ref, send, values, table, product, arrived):
    table_copy = pltpu.make_async_copy(table_ref, table, arrived.at[8])
    table_copy.start()
    copies = [pltpu.make_async_copy(field.at[:, g], values.at[g], arrived.at[g]) for g in range(8)]
    for copy in copies:
        copy.start()
    table_copy.wait()
    for g in range(8):
        copies[g].wait()
        rows = jnp.concatenate([values[g, h] for h in range(4)], axis=1)
        product[g] = dot(rows, table[...])
    spread_groups(product, send, 128)


def columns_fine_kernel(received, table, send, lines):
    for pair in range(8):
        block = received[:, 16 * pair : 16 * pair + 16, :].astype(F32).reshape(16, 2, 8, 128)
        data = jnp.concatenate([block[:, e].reshape(128, 128) for e in range(2)], axis=1)
        out = dot(table[...], data.astype(BF16))
        out = out[:KEPT] + turn(out[KEPT:])
        for e in range(2):
            lines[pl.ds(2 * pair + e, KEPT, stride=16), :] = out[:, 128 * e : 128 * e + 128]
    send[...] = lines[...].reshape(8, 64, 128).astype(BF16)


def columns_coarse_kernel(received, table, send, cells, lines):
    cells[...] = received[...].astype(F32).reshape(512, 128)
    data = jnp.concatenate([cells[pl.ds(x, 64, stride=8), :] for x in range(8)], axis=1)
    out = dot(table[...], data.astype(BF16))
    out = out[:KEPT] + turn(out[KEPT:])
    for x in range(8):
        lines[pl.ds(x, KEPT, stride=8), :] = out[:, 128 * x : 128 * x + 128]
    send[...] = lines[...].reshape(8, 32, 128).astype(BF16)


def mix_kernel(received, forward, inverse, weights, send, modes, mixed):
    own = received.shape[2]
    data = received[...].astype(F32)
    data = jnp.concatenate([data[:, m].reshape(8 * own, 128) for m in range(4)], axis=1)
    out = dot(forward[...], data.astype(BF16))
    out = out[:KEPT] + turn(out[KEPT:])
    out = jnp.concatenate([out[:, 128 * m : 128 * m + 128] for m in range(4)], axis=0)
    modes[...] = out.T

    def step(g, sums):
        sums = list(sums)
        base = g * 16
        for h in range(4):
            for k in range(2):
                real = modes[pl.ds(base + 4 * k + h, 1), :]
                imag = modes[pl.ds(base + 8 + 4 * k + h, 1), :]
                w_real = weights[0, 8 * h + g, k].astype(F32)
                w_imag = weights[1, 8 * h + g, k].astype(F32)
                sums[2 * k] = sums[2 * k] + (w_real * real - w_imag * imag)
                sums[2 * k + 1] = sums[2 * k + 1] + (w_real * imag + w_imag * real)
        return tuple(sums)

    sums = lax.fori_loop(0, 8, step, tuple(jnp.zeros((C, 128), F32) for _ in range(4)))
    for k in range(2):
        for r in range(2):
            for h in range(4):
                mixed[pl.ds(8 * r + 4 * k + h, 8, stride=16), :] = sums[2 * k + r][8 * h : 8 * h + 8]
    back = mixed[...].T
    back = jnp.concatenate([back[32 * m : 32 * m + 32] for m in range(4)], axis=1)
    back = jnp.concatenate([back, turn(back)], axis=0).astype(BF16)
    out = dot(inverse[...], jnp.concatenate([back, back], axis=0))
    for m in range(4):
        send[:, m] = out[:, 128 * m : 128 * m + 128].reshape(8, own, 128).astype(BF16)


def back_columns(lines, table, own, first, count):
    data = jnp.concatenate([lines[pl.ds(first + x, KEPT, stride=own), :] for x in range(count)], axis=1)
    data = jnp.concatenate([data, turn(data)], axis=0).astype(BF16)
    return dot(table, jnp.concatenate([data, data], axis=0))


def back_fine_kernel(received, table, send, lines):
    lines[...] = received[...].astype(F32).reshape(512, 128)
    for pair in range(8):
        out = back_columns(lines, table[...], 16, 2 * pair, 2)
        parts = [out[:, 128 * e : 128 * e + 128].reshape(16, 1, 8, 128) for e in range(2)]
        block = jnp.concatenate(parts, axis=1).reshape(16, 16, 128)
        send[:, 16 * pair : 16 * pair + 16, :] = block.astype(BF16)


def back_coarse_kernel(received, table, send, lines, cells):
    lines[...] = received[...].astype(F32).reshape(256, 128)
    out = back_columns(lines, table[...], 8, 0, 8)
    for x in range(8):
        cells[pl.ds(x, 64, stride=8), :] = out[:, 128 * x : 128 * x + 128]
    send[...] = cells[...].reshape(16, 32, 128).astype(BF16)


def channel_map(mixing):
    row = lax.broadcasted_iota(jnp.int32, (512, C), 0)
    channel = lax.broadcasted_iota(jnp.int32, (512, C), 1)
    pick = jnp.where((row >> 4) == channel, 1.0, 0.0).astype(BF16)
    wide = lax.dot_general(pick, mixing, (((1,), (1,)), ((), ())), preferred_element_type=F32)
    wide = lax.dot_general(wide.astype(BF16), pick, (((1,), (1,)), ((), ())), preferred_element_type=F32)
    a = lax.broadcasted_iota(jnp.int32, (512, 512), 0)
    b = lax.broadcasted_iota(jnp.int32, (512, 512), 1)
    return jnp.where(((a ^ b) & 15) == 0, wide, 0.0).astype(BF16)


def pointwise_kernel(field, mix_fine, bias, mix_coarse, total, map_coarse):
    channels = channel_map(mix_fine[...])
    for p in range(8):
        out = dot(channels, field[:, 16 * p : 16 * p + 16, :].reshape(512, 128)).reshape(C, 16, 128)
        for o in range(C):
            total[o, 16 * p : 16 * p + 16, :] = out[o] + bias[o]
    map_coarse[...] = channel_map(mix_coarse[...])


def gelu(v):
    inner = v * (0.7978845608028654 + 0.03567740813636141 * (v * v))
    half = 0.5 * v
    return half + half * jnp.tanh(inner)


def upper_kernel(received, table, total, next_table, upper, pooled, send, spread, sums, product):
    collect_groups(received, spread, 128)
    even = (lanes_of((64, 128)) & 1) == 0
    for g in range(8):
        out = dot(spread[g], table[...])
        for h in range(4):
            o = 8 * h + g
            value = gelu(out[:, 128 * h : 128 * h + 128] + total[o]).astype(BF16)
            upper[o] = value
            value = value.astype(F32).reshape(8, 2, 8, 128)
            value = (value[:, 0] + value[:, 1]).reshape(64, 128)
            sums[o] = value + jnp.where(even, pltpu.roll(value, 127, 1), pltpu.roll(value, 1, 1))
    for o in range(C):
        parts = [sums[o, pl.ds(2 * y, 8, stride=8), :] + sums[o, pl.ds(2 * y + 1, 8, stride=8), :] for y in range(4)]
        pooled[o] = (jnp.concatenate(parts, axis=0) * 0.125).astype(BF16)
    for g in range(8):
        rows = jnp.concatenate([pooled[8 * h + g] for h in range(4)], axis=1)
        product[g] = dot(rows, next_table[...])
    spread_groups(product, send, 32)


def lower_kernel(received, table, pooled, channels, bias, upper, out_ref, spread, total, sums, merged, left):
    blocks = [pooled[:, 16 * p : 16 * p + 16, :].reshape(512, 128) for p in range(2)]
    own = dot(channels[...], jnp.concatenate(blocks, axis=1))
    for p in range(2):
        total[:, 16 * p : 16 * p + 16, :] = own[:, 128 * p : 128 * p + 128].reshape(C, 16, 128)
    collect_groups(received, spread, 32)
    copies = [pltpu.make_async_copy(merged.at[g], out_ref.at[:, g], left.at[g]) for g in range(8)]
    for g in range(8):
        out = dot(spread[g], table[...])
        for h in range(4):
            o = 8 * h + g
            value = gelu(out[:, 128 * h : 128 * h + 128] + total[o] + bias[o]).astype(BF16).astype(F32)
            for y in range(4):
                part = value[8 * y : 8 * y + 8]
                sums[o, pl.ds(2 * y, 8, stride=8), :] = part
                sums[o, pl.ds(2 * y + 1, 8, stride=8), :] = part
            added = sums[o].reshape(8, 1, 8, 128)
            fine = upper[o].astype(F32).reshape(8, 2, 8, 128)
            merged[g, h] = (fine + added).reshape(128, 128).astype(BF16)
        copies[g].start()
    for copy in copies:
        copy.wait()


VMEM = pl.BlockSpec(memory_space=pltpu.VMEM)
SMEM = pl.BlockSpec(memory_space=pltpu.SMEM)
HBM = pl.BlockSpec(memory_space=pltpu.HBM)


def call(kernel, outs, *operands, scratch=(), specs=None, out_specs=None, limit=8):
    shapes = [jax.ShapeDtypeStruct(shape, kind) for shape, kind in outs]
    out_specs = out_specs or [VMEM] * len(shapes)
    return pl.pallas_call(
        kernel,
        out_shape=shapes if len(shapes) > 1 else shapes[0],
        in_specs=specs or [VMEM] * len(operands),
        out_specs=out_specs if len(shapes) > 1 else out_specs[0],
        scratch_shapes=[pltpu.VMEM(*s) if isinstance(s, tuple) else s for s in scratch],
        compiler_params=pltpu.CompilerParams(vmem_limit_bytes=limit << 20),
    )(*operands)


def exchange(x, axis):
    return lax.all_to_all(x, axis, 0, 0, tiled=True)


def lay_out(spectral):
    place = jnp.asarray(np.eye(128).reshape(4, 32, 128).astype(BF16))
    return jnp.einsum("riojmk,mjl->rikol", spectral, place, preferred_element_type=BF16)


def on_device(field, spec_fine, mix_fine, bias_fine, spec_coarse, mix_coarse, bias_coarse):
    field = field.reshape(C, 128, 128)
    forward_fine, inverse_fine = jnp.asarray(plane_forward(128)), jnp.asarray(plane_inverse(128))
    forward_coarse, inverse_coarse = jnp.asarray(plane_forward(64)), jnp.asarray(plane_inverse(64))

    x = call(
        depth_kernel,
        [((16, 128, 128), BF16)],
        field.reshape(4, 8, 128, 128),
        jnp.asarray(depth_forward(128, 1)),
        specs=[HBM, HBM],
        scratch=[
            ((8, 4, 128, 128), BF16),
            ((512, 256), BF16),
            ((8, 128, 256), F32),
            pltpu.SemaphoreType.DMA((9,)),
        ],
    )
    x = exchange(x, "py")
    weights_fine = lay_out(spec_fine)
    weights_coarse = lay_out(spec_coarse)
    total, map_coarse = call(
        pointwise_kernel,
        [((C, 128, 128), F32), ((512, 512), BF16)],
        field,
        mix_fine,
        bias_fine,
        mix_coarse,
        specs=[VMEM, VMEM, SMEM, VMEM],
    )
    x, weights_fine, weights_coarse, total, map_coarse = lax.optimization_barrier(
        (x, weights_fine, weights_coarse, total, map_coarse)
    )
    x = call(columns_fine_kernel, [((8, 64, 128), BF16)], x, forward_fine, scratch=[((512, 128), F32)])
    x = exchange(x, "px").reshape(8, 4, 16, 128)
    mix_scratch = [((128, 128), F32), ((128, 128), F32)]
    x = call(mix_kernel, [((8, 4, 16, 128), BF16)], x, forward_fine, inverse_fine, weights_fine, scratch=mix_scratch)
    x = exchange(x.reshape(8, 64, 128), "px")
    x = call(back_fine_kernel, [((16, 128, 128), BF16)], x, inverse_fine, scratch=[((512, 128), F32)])
    x = exchange(x, "py")
    upper, pooled, x = call(
        upper_kernel,
        [((C, 128, 128), BF16), ((C, 32, 128), BF16), ((16, 32, 128), BF16)],
        x,
        jnp.asarray(depth_inverse(128, 1)),
        total,
        jnp.asarray(depth_forward(64, 2)),
        scratch=[((8, 128, 256), BF16), ((C, 64, 128), F32), ((8, 32, 256), F32)],
        limit=12,
    )
    x = exchange(x, "py")
    scratch = [((512, 128), F32), ((256, 128), F32)]
    x = call(columns_coarse_kernel, [((8, 32, 128), BF16)], x, forward_coarse, scratch=scratch)
    x = exchange(x, "px").reshape(8, 4, 8, 128)
    x = call(mix_kernel, [((8, 4, 8, 128), BF16)], x, forward_coarse, inverse_coarse, weights_coarse, scratch=mix_scratch)
    x = exchange(x.reshape(8, 32, 128), "px")
    x = call(back_coarse_kernel, [((16, 32, 128), BF16)], x, inverse_coarse, scratch=scratch[::-1])
    x = exchange(x, "py")
    out = call(
        lower_kernel,
        [((4, 8, 128, 128), BF16)],
        x,
        jnp.asarray(depth_inverse(64, 2)),
        pooled,
        map_coarse,
        bias_coarse,
        upper,
        specs=[VMEM, VMEM, VMEM, VMEM, SMEM, VMEM],
        out_specs=[HBM],
        scratch=[
            ((8, 32, 256), BF16),
            ((C, 32, 128), F32),
            ((C, 64, 128), F32),
            ((8, 4, 128, 128), BF16),
            pltpu.SemaphoreType.DMA((8,)),
        ],
        limit=12,
    )
    return out.reshape(C, 16, 8, 128)


def solution(mesh):
    return jax.shard_map(
        on_device,
        mesh=mesh,
        in_specs=(
            P(None, "px", "py", None),
            P(None, None, None, None, "px", "py"),
            P(),
            P(),
            P(None, None, None, None, "px", "py"),
            P(),
            P(),
        ),
        out_specs=P(None, "px", "py", None),
        check_vma=False,
    )
```

```python
import functools
import math

import jax
import jax.numpy as jnp
import numpy as np
from jax import lax
from jax.experimental import pallas as pl
from jax.experimental.pallas import tpu as pltpu
from jax.sharding import PartitionSpec as P

C = 32
KEPT = 32
F32 = jnp.float32
BF16 = jnp.bfloat16


def angles(cells, offset):
    windings = np.arange(cells)[:, None] * (np.arange(KEPT)[None, :] - offset) % cells
    return windings.astype(np.float64) * (2.0 * math.pi / cells)


def depth_forward(cells, repeat):
    angle = angles(cells, 0)
    table = np.stack([np.cos(angle), -np.sin(angle)])
    table = table.reshape(2, cells, 16, 2).transpose(1, 2, 0, 3)
    spread = np.zeros((cells, repeat) + table.shape[1:])
    spread[:, 0] = table
    spread = spread.reshape((cells * repeat,) + table.shape[1:])
    result = np.einsum("zprk,hg->hzprkg", spread, np.eye(4))
    return result.reshape(4 * cells * repeat, 256).astype(BF16)


def plane_forward(cells):
    angle = angles(cells, KEPT // 2)
    return np.concatenate([np.cos(angle), -np.sin(angle)], axis=1).T.astype(BF16)


def halves(table):
    high = table.astype(np.float32).astype(BF16)
    low = (table.astype(np.float32) - high.astype(np.float32)).astype(BF16)
    return high, low


def plane_inverse(cells):
    angle = angles(cells, KEPT // 2)
    high, low = halves(np.concatenate([np.cos(angle), np.sin(angle)], axis=1))
    return np.concatenate([high, low], axis=1)


def depth_inverse(cells, repeat):
    angle = angles(cells, 0)
    factor = np.where(np.arange(KEPT) == 0, 1.0, 2.0) / float(cells**3)
    table = np.stack([factor * np.cos(angle), -factor * np.sin(angle)])
    table = np.repeat(table, repeat, axis=1).reshape(2, cells * repeat, 16, 2)
    result = np.einsum("rzpk,hg->prkhgz", table, np.eye(4)).reshape(256, 4 * cells * repeat)
    return result.astype(BF16)


def dot(a, b):
    return jnp.dot(a, b, preferred_element_type=F32)


def lanes_of(shape):
    return lax.broadcasted_iota(jnp.int32, shape, len(shape) - 1)


def turn(x):
    width = x.shape[-1]
    real = (lanes_of(x.shape) & 8) == 0
    return jnp.where(real, -pltpu.roll(x, width - 8, 1), pltpu.roll(x, 8, 1))


def swap_blocks(parts):
    parts = list(parts)
    lane = lanes_of(parts[0].shape)
    for step in (1, 2, 4):
        keep = (lane & (16 * step)) == 0
        for low in range(8):
            if low & step == 0:
                a, b = parts[low], parts[low + step]
                parts[low] = jnp.where(keep, a, pltpu.roll(b, 16 * step, 1))
                parts[low + step] = jnp.where(keep, pltpu.roll(a, 128 - 16 * step, 1), b)
    return parts


def spread_groups(product, send, rows, sent=None):
    def chunk(index, carry):
        at = pl.ds(pl.multiple_of(index * 16, 16), 16)
        for half in range(2):
            parts = swap_blocks([product[g, at, 128 * half : 128 * half + 128] for g in range(8)])
            for b in range(8):
                send[8 * half + b, at, :] = parts[b].astype(BF16)
        if sent is not None:
            sent(index, at)
        return carry

    lax.fori_loop(0, rows // 16, chunk, 0)


def collect_groups(received, spread, rows):
    def chunk(index, carry):
        at = pl.ds(pl.multiple_of(index * 16, 16), 16)
        for half in range(2):
            parts = swap_blocks([received[8 * half + b, at, :].astype(F32) for b in range(8)])
            for g in range(8):
                spread[g, at, 128 * half : 128 * half + 128] = parts[g].astype(BF16)
        return carry

    lax.fori_loop(0, rows // 16, chunk, 0)


def depth_kernel(field, table_ref, send_ref, values, table, product, send, arrived, left):
    copies = [pltpu.make_async_copy(field.at[:, g], values.at[g], arrived.at[g]) for g in range(8)]
    table_copy = pltpu.make_async_copy(table_ref, table, arrived.at[8])
    copies[0].start()
    table_copy.start()
    for copy in copies[1:]:
        copy.start()
    table_copy.wait()
    for g in range(8):
        copies[g].wait()
        rows = jnp.concatenate([values[g, h] for h in range(4)], axis=1)
        product[g] = dot(rows, table[...])

    def leave(index, at):
        pltpu.make_async_copy(send.at[:, at, :], send_ref.at[:, at, :], left.at[index]).start()

    spread_groups(product, send, 128, leave)
    for index in range(8):
        at = pl.ds(16 * index, 16)
        pltpu.make_async_copy(send.at[:, at, :], send_ref.at[:, at, :], left.at[index]).wait()


def columns_fine_kernel(received, table, send, lines):
    for pair in range(8):
        block = received[:, 16 * pair : 16 * pair + 16, :].astype(F32).reshape(16, 2, 8, 128)
        data = jnp.concatenate([block[:, e].reshape(128, 128) for e in range(2)], axis=1)
        out = dot(table[...], data.astype(BF16))
        out = out[:KEPT] + turn(out[KEPT:])
        for e in range(2):
            lines[pl.ds(2 * pair + e, KEPT, stride=16), :] = out[:, 128 * e : 128 * e + 128]
    send[...] = lines[...].reshape(8, 64, 128).astype(BF16)


def columns_coarse_kernel(received, table, send, cells, lines):
    cells[...] = received[...].astype(F32).reshape(512, 128)
    data = jnp.concatenate([cells[pl.ds(x, 64, stride=8), :] for x in range(8)], axis=1)
    out = dot(table[...], data.astype(BF16))
    out = out[:KEPT] + turn(out[KEPT:])
    for x in range(8):
        lines[pl.ds(x, KEPT, stride=8), :] = out[:, 128 * x : 128 * x + 128]
    send[...] = lines[...].reshape(8, 32, 128).astype(BF16)


def mix_kernel(received, forward, inverse, weights_ref, send, modes, mixed, weights=None, arrived=None):
    def weight_copy(g):
        return pltpu.make_async_copy(weights_ref.at[:, :, g], weights.at[:, :, g], arrived.at[g])

    if weights is None:
        weights = weights_ref
    else:
        for g in range(8):
            weight_copy(g).start()
    own = received.shape[2]
    data = received[...].astype(F32)
    data = jnp.concatenate([data[:, m].reshape(8 * own, 128) for m in range(4)], axis=1)
    out = dot(forward[...], data.astype(BF16))
    out = out[:KEPT] + turn(out[KEPT:])
    out = jnp.concatenate([out[:, 128 * m : 128 * m + 128] for m in range(4)], axis=0)
    modes[...] = out.T

    def step(g, sums):
        if arrived is not None:
            weight_copy(g).wait()
        sums = list(sums)
        base = g * 16
        for h in range(4):
            for k in range(2):
                real = modes[pl.ds(base + 4 * k + h, 1), :]
                imag = modes[pl.ds(base + 8 + 4 * k + h, 1), :]
                w_real = weights[0, h, g, k].astype(F32)
                w_imag = weights[1, h, g, k].astype(F32)
                sums[2 * k] = sums[2 * k] + (w_real * real - w_imag * imag)
                sums[2 * k + 1] = sums[2 * k + 1] + (w_real * imag + w_imag * real)
        return tuple(sums)

    sums = lax.fori_loop(0, 8, step, tuple(jnp.zeros((C, 128), F32) for _ in range(4)))
    for k in range(2):
        for r in range(2):
            for h in range(4):
                mixed[pl.ds(8 * r + 4 * k + h, 8, stride=16), :] = sums[2 * k + r][8 * h : 8 * h + 8]
    back = mixed[...].T
    back = jnp.concatenate([back[32 * m : 32 * m + 32] for m in range(4)], axis=1)
    back = jnp.concatenate([back, turn(back)], axis=0).astype(BF16)
    out = dot(inverse[...], jnp.concatenate([back, back], axis=0))
    for m in range(4):
        send[:, m] = out[:, 128 * m : 128 * m + 128].reshape(8, own, 128).astype(BF16)


def back_columns(lines, table, own, first, count):
    data = jnp.concatenate([lines[pl.ds(first + x, KEPT, stride=own), :] for x in range(count)], axis=1)
    data = jnp.concatenate([data, turn(data)], axis=0).astype(BF16)
    return dot(table, jnp.concatenate([data, data], axis=0))


def back_fine_kernel(received, table, send, lines):
    lines[...] = received[...].astype(F32).reshape(512, 128)
    for pair in range(8):
        out = back_columns(lines, table[...], 16, 2 * pair, 2)
        parts = [out[:, 128 * e : 128 * e + 128].reshape(16, 1, 8, 128) for e in range(2)]
        block = jnp.concatenate(parts, axis=1).reshape(16, 16, 128)
        send[:, 16 * pair : 16 * pair + 16, :] = block.astype(BF16)


def back_coarse_kernel(received, table, send, lines, cells):
    lines[...] = received[...].astype(F32).reshape(256, 128)
    out = back_columns(lines, table[...], 8, 0, 8)
    for x in range(8):
        cells[pl.ds(x, 64, stride=8), :] = out[:, 128 * x : 128 * x + 128]
    send[...] = cells[...].reshape(16, 32, 128).astype(BF16)


def channel_map(mixing):
    row = lax.broadcasted_iota(jnp.int32, (512, C), 0)
    channel = lax.broadcasted_iota(jnp.int32, (512, C), 1)
    pick = jnp.where((row >> 4) == channel, 1.0, 0.0).astype(BF16)
    wide = lax.dot_general(pick, mixing, (((1,), (1,)), ((), ())), preferred_element_type=F32)
    wide = lax.dot_general(wide.astype(BF16), pick, (((1,), (1,)), ((), ())), preferred_element_type=F32)
    a = lax.broadcasted_iota(jnp.int32, (512, 512), 0)
    b = lax.broadcasted_iota(jnp.int32, (512, 512), 1)
    return jnp.where(((a ^ b) & 15) == 0, wide, 0.0).astype(BF16)


def pointwise_kernel(field, mix_fine, bias, mix_coarse, total, map_coarse):
    channels = channel_map(mix_fine[...])
    for pair in range(4):
        rows = [slice(32 * pair + 16 * e, 32 * pair + 16 * e + 16) for e in range(2)]
        out = dot(channels, jnp.concatenate([field[:, at, :].reshape(512, 128) for at in rows], axis=1))
        for o in range(C):
            for e in range(2):
                total[o, rows[e], :] = out[16 * o : 16 * o + 16, 128 * e : 128 * e + 128] + bias[o]
    map_coarse[...] = channel_map(mix_coarse[...])


def gelu(v):
    inner = v * (0.7978845608028654 + 0.03567740813636141 * (v * v))
    half = 0.5 * v
    return half + half * jnp.tanh(inner)


def upper_kernel(received, table, total, next_table, upper, pooled, send, spread, sums, product):
    collect_groups(received, spread, 128)
    even = (lanes_of((64, 128)) & 1) == 0
    for g in range(8):
        out = dot(spread[g], table[...])
        for h in range(4):
            o = 8 * h + g
            value = gelu(out[:, 128 * h : 128 * h + 128] + total[o]).astype(BF16)
            upper[o] = value
            value = value.astype(F32).reshape(8, 2, 8, 128)
            value = (value[:, 0] + value[:, 1]).reshape(64, 128)
            sums[o] = value + jnp.where(even, pltpu.roll(value, 127, 1), pltpu.roll(value, 1, 1))
    for o in range(C):
        parts = [sums[o, pl.ds(2 * y, 8, stride=8), :] + sums[o, pl.ds(2 * y + 1, 8, stride=8), :] for y in range(4)]
        pooled[o] = (jnp.concatenate(parts, axis=0) * 0.125).astype(BF16)
    for g in range(8):
        rows = jnp.concatenate([pooled[8 * h + g] for h in range(4)], axis=1)
        product[g] = dot(rows, next_table[...])
    spread_groups(product, send, 32)


def lower_kernel(received, table, pooled, channels, bias, upper, out_ref, spread, total, sums, merged, left):
    blocks = [pooled[:, 16 * p : 16 * p + 16, :].reshape(512, 128) for p in range(2)]
    own = dot(channels[...], jnp.concatenate(blocks, axis=1))
    for p in range(2):
        total[:, 16 * p : 16 * p + 16, :] = own[:, 128 * p : 128 * p + 128].reshape(C, 16, 128)
    collect_groups(received, spread, 32)
    copies = [pltpu.make_async_copy(merged.at[g], out_ref.at[:, g], left.at[g]) for g in range(8)]
    for g in range(8):
        out = dot(spread[g], table[...])
        for h in range(4):
            o = 8 * h + g
            value = gelu(out[:, 128 * h : 128 * h + 128] + total[o] + bias[o]).astype(BF16).astype(F32)
            for y in range(4):
                part = value[8 * y : 8 * y + 8]
                sums[o, pl.ds(2 * y, 8, stride=8), :] = part
                sums[o, pl.ds(2 * y + 1, 8, stride=8), :] = part
            added = sums[o].reshape(8, 1, 8, 128)
            fine = upper[o].astype(F32).reshape(8, 2, 8, 128)
            merged[g, h] = (fine + added).reshape(128, 128).astype(BF16)
        copies[g].start()
    for copy in copies:
        copy.wait()


VMEM = pl.BlockSpec(memory_space=pltpu.VMEM)
SMEM = pl.BlockSpec(memory_space=pltpu.SMEM)
HBM = pl.BlockSpec(memory_space=pltpu.HBM)


def call(kernel, outs, *operands, scratch=(), specs=None, out_specs=None, limit=8):
    shapes = [jax.ShapeDtypeStruct(shape, kind) for shape, kind in outs]
    out_specs = out_specs or [VMEM] * len(shapes)
    return pl.pallas_call(
        kernel,
        out_shape=shapes if len(shapes) > 1 else shapes[0],
        in_specs=specs or [VMEM] * len(operands),
        out_specs=out_specs if len(shapes) > 1 else out_specs[0],
        scratch_shapes=[pltpu.VMEM(*s) if isinstance(s, tuple) else s for s in scratch],
        compiler_params=pltpu.CompilerParams(vmem_limit_bytes=limit << 20),
    )(*operands)


hold = pltpu.with_memory_space_constraint


def exchange(x, axis):
    return lax.all_to_all(x, axis, 0, 0, tiled=True)


def lay_out(spectral):
    place = jnp.asarray(np.eye(128).reshape(4, 32, 128).astype(BF16))
    return jnp.einsum("riojmk,mjl->rikol", spectral, place, preferred_element_type=BF16)


def on_device(field, spec_fine, mix_fine, bias_fine, spec_coarse, mix_coarse, bias_coarse):
    field = field.reshape(C, 128, 128)
    forward_fine, inverse_fine = jnp.asarray(plane_forward(128)), jnp.asarray(plane_inverse(128))
    forward_coarse, inverse_coarse = jnp.asarray(plane_forward(64)), jnp.asarray(plane_inverse(64))

    x = call(
        depth_kernel,
        [((16, 128, 128), BF16)],
        hold(field.reshape(4, 8, 128, 128), pltpu.HBM),
        hold(jnp.asarray(depth_forward(128, 1)), pltpu.HBM),
        specs=[HBM, HBM],
        out_specs=[HBM],
        scratch=[
            ((8, 4, 128, 128), BF16),
            ((512, 256), BF16),
            ((8, 128, 256), F32),
            ((16, 128, 128), BF16),
            pltpu.SemaphoreType.DMA((9,)),
            pltpu.SemaphoreType.DMA((8,)),
        ],
    )
    x = exchange(x, "py")
    weights_fine = lay_out(spec_fine)
    spec_coarse, weights_fine = lax.optimization_barrier((spec_coarse, weights_fine))
    weights_coarse = lay_out(spec_coarse)
    field, weights_coarse = lax.optimization_barrier((field, weights_coarse))
    total, map_coarse = call(
        pointwise_kernel,
        [((C, 128, 128), F32), ((512, 512), BF16)],
        field,
        mix_fine,
        bias_fine,
        mix_coarse,
        specs=[VMEM, VMEM, SMEM, VMEM],
    )
    x, weights_fine, weights_coarse, total, map_coarse = lax.optimization_barrier(
        (x, weights_fine, weights_coarse, total, map_coarse)
    )
    weights_fine = hold(weights_fine.reshape(2, 4, 8, 2, C, 128), pltpu.HBM)
    weights_coarse = weights_coarse.reshape(2, 4, 8, 2, C, 128)
    x = call(columns_fine_kernel, [((8, 64, 128), BF16)], x, forward_fine, scratch=[((512, 128), F32)])
    x = exchange(x, "px").reshape(8, 4, 16, 128)
    mix_scratch = [((128, 128), F32), ((128, 128), F32)]
    own_weights = [((2, 4, 8, 2, C, 128), BF16), pltpu.SemaphoreType.DMA((8,))]
    x = call(mix_kernel, [((8, 4, 16, 128), BF16)], x, forward_fine, inverse_fine, weights_fine, specs=[VMEM, VMEM, VMEM, HBM], scratch=mix_scratch + own_weights)
    x = exchange(x.reshape(8, 64, 128), "px")
    x = call(back_fine_kernel, [((16, 128, 128), BF16)], x, inverse_fine, scratch=[((512, 128), F32)])
    x = exchange(x, "py")
    upper, pooled, x = call(
        upper_kernel,
        [((C, 128, 128), BF16), ((C, 32, 128), BF16), ((16, 32, 128), BF16)],
        x,
        jnp.asarray(depth_inverse(128, 1)),
        total,
        jnp.asarray(depth_forward(64, 2)),
        scratch=[((8, 128, 256), BF16), ((C, 64, 128), F32), ((8, 32, 256), F32)],
        limit=12,
    )
    x = exchange(x, "py")
    scratch = [((512, 128), F32), ((256, 128), F32)]
    x = call(columns_coarse_kernel, [((8, 32, 128), BF16)], x, forward_coarse, scratch=scratch)
    x = exchange(x, "px").reshape(8, 4, 8, 128)
    x = call(mix_kernel, [((8, 4, 8, 128), BF16)], x, forward_coarse, inverse_coarse, weights_coarse, scratch=mix_scratch)
    x = exchange(x.reshape(8, 32, 128), "px")
    x = call(back_coarse_kernel, [((16, 32, 128), BF16)], x, inverse_coarse, scratch=scratch[::-1])
    x = exchange(x, "py")
    out = call(
        lower_kernel,
        [((4, 8, 128, 128), BF16)],
        x,
        jnp.asarray(depth_inverse(64, 2)),
        pooled,
        map_coarse,
        bias_coarse,
        upper,
        specs=[VMEM, VMEM, VMEM, VMEM, SMEM, VMEM],
        out_specs=[HBM],
        scratch=[
            ((8, 32, 256), BF16),
            ((C, 32, 128), F32),
            ((C, 64, 128), F32),
            ((8, 4, 128, 128), BF16),
            pltpu.SemaphoreType.DMA((8,)),
        ],
        limit=12,
    )
    return out.reshape(C, 16, 8, 128)


def solution(mesh):
    return jax.shard_map(
        on_device,
        mesh=mesh,
        in_specs=(
            P(None, "px", "py", None),
            P(None, None, None, None, "px", "py"),
            P(),
            P(),
            P(None, None, None, None, "px", "py"),
            P(),
            P(),
        ),
        out_specs=P(None, "px", "py", None),
        check_vma=False,
    )
```

```python
import functools
import math

import jax
import jax.numpy as jnp
import numpy as np
from jax import lax
from jax.experimental import pallas as pl
from jax.experimental.pallas import tpu as pltpu
from jax.sharding import PartitionSpec as P

C = 32
KEPT = 32
F32 = jnp.float32
BF16 = jnp.bfloat16


def angles(cells, offset):
    windings = np.arange(cells)[:, None] * (np.arange(KEPT)[None, :] - offset) % cells
    return windings.astype(np.float64) * (2.0 * math.pi / cells)


def depth_forward(cells, repeat):
    angle = angles(cells, 0)
    table = np.stack([np.cos(angle), -np.sin(angle)])
    table = table.reshape(2, cells, 16, 2).transpose(1, 2, 0, 3)
    spread = np.zeros((cells, repeat) + table.shape[1:])
    spread[:, 0] = table
    spread = spread.reshape((cells * repeat,) + table.shape[1:])
    result = np.einsum("zprk,hg->hzprkg", spread, np.eye(4))
    return result.reshape(4 * cells * repeat, 256).astype(BF16)


def plane_forward(cells):
    angle = angles(cells, KEPT // 2)
    return np.concatenate([np.cos(angle), -np.sin(angle)], axis=1).T.astype(BF16)


def halves(table):
    high = table.astype(np.float32).astype(BF16)
    low = (table.astype(np.float32) - high.astype(np.float32)).astype(BF16)
    return high, low


def plane_inverse(cells):
    angle = angles(cells, KEPT // 2)
    high, low = halves(np.concatenate([np.cos(angle), np.sin(angle)], axis=1))
    return np.concatenate([high, low], axis=1)


def depth_inverse(cells, repeat):
    angle = angles(cells, 0)
    factor = np.where(np.arange(KEPT) == 0, 1.0, 2.0) / float(cells**3)
    table = np.stack([factor * np.cos(angle), -factor * np.sin(angle)])
    table = np.repeat(table, repeat, axis=1).reshape(2, cells * repeat, 16, 2)
    result = np.einsum("rzpk,hg->prkhgz", table, np.eye(4)).reshape(256, 4 * cells * repeat)
    return result.astype(BF16)


def dot(a, b):
    return jnp.dot(a, b, preferred_element_type=F32)


def lanes_of(shape):
    return lax.broadcasted_iota(jnp.int32, shape, len(shape) - 1)


def turn(x):
    width = x.shape[-1]
    real = (lanes_of(x.shape) & 8) == 0
    return jnp.where(real, -pltpu.roll(x, width - 8, 1), pltpu.roll(x, 8, 1))


def swap_blocks(parts):
    parts = list(parts)
    lane = lanes_of(parts[0].shape)
    for step in (1, 2, 4):
        keep = (lane & (16 * step)) == 0
        for low in range(8):
            if low & step == 0:
                a, b = parts[low], parts[low + step]
                parts[low] = jnp.where(keep, a, pltpu.roll(b, 16 * step, 1))
                parts[low + step] = jnp.where(keep, pltpu.roll(a, 128 - 16 * step, 1), b)
    return parts


def spread_groups(product, send, rows, sent=None):
    def chunk(index, carry):
        at = pl.ds(pl.multiple_of(index * 16, 16), 16)
        for half in range(2):
            parts = swap_blocks([product[g, at, 128 * half : 128 * half + 128] for g in range(8)])
            for b in range(8):
                send[8 * half + b, at, :] = parts[b].astype(BF16)
        if sent is not None:
            sent(index, at)
        return carry

    lax.fori_loop(0, rows // 16, chunk, 0, unroll=min(2, rows // 16))


def collect_groups(received, spread, rows):
    def chunk(index, carry):
        at = pl.ds(pl.multiple_of(index * 16, 16), 16)
        for half in range(2):
            parts = swap_blocks([received[8 * half + b, at, :].astype(F32) for b in range(8)])
            for g in range(8):
                spread[g, at, 128 * half : 128 * half + 128] = parts[g].astype(BF16)
        return carry

    lax.fori_loop(0, rows // 16, chunk, 0, unroll=min(2, rows // 16))


def depth_kernel(field, table_ref, send_ref, values, table, product, send, arrived, left):
    copies = [pltpu.make_async_copy(field.at[:, g], values.at[g], arrived.at[g]) for g in range(8)]
    table_copy = pltpu.make_async_copy(table_ref, table, arrived.at[8])
    copies[0].start()
    table_copy.start()
    for copy in copies[1:]:
        copy.start()
    table_copy.wait()

    def group(pair, carry):
        for e in range(2):
            g = 2 * pair + e
            pltpu.make_async_copy(field.at[:, g], values.at[g], arrived.at[g]).wait()
        for e in range(2):
            rows = jnp.concatenate([values[2 * pair + e, h] for h in range(4)], axis=1)
            product[2 * pair + e] = dot(rows, table[...])
        return carry

    lax.fori_loop(0, 4, group, 0)

    def leave(index, at):
        pltpu.make_async_copy(send.at[:, at, :], send_ref.at[:, at, :], left.at[index]).start()

    spread_groups(product, send, 128, leave)
    for index in range(8):
        at = pl.ds(16 * index, 16)
        pltpu.make_async_copy(send.at[:, at, :], send_ref.at[:, at, :], left.at[index]).wait()


def columns_fine_kernel(received, table, send, lines):
    for pair in range(8):
        block = received[:, 16 * pair : 16 * pair + 16, :].astype(F32).reshape(16, 2, 8, 128)
        data = jnp.concatenate([block[:, e].reshape(128, 128) for e in range(2)], axis=1)
        out = dot(table[...], data.astype(BF16))
        out = out[:KEPT] + turn(out[KEPT:])
        for e in range(2):
            lines[pl.ds(2 * pair + e, KEPT, stride=16), :] = out[:, 128 * e : 128 * e + 128]
    send[...] = lines[...].reshape(8, 64, 128).astype(BF16)


def columns_coarse_kernel(received, table, send, cells, lines):
    cells[...] = received[...].astype(F32).reshape(512, 128)
    data = jnp.concatenate([cells[pl.ds(x, 64, stride=8), :] for x in range(8)], axis=1)
    out = dot(table[...], data.astype(BF16))
    out = out[:KEPT] + turn(out[KEPT:])
    for x in range(8):
        lines[pl.ds(x, KEPT, stride=8), :] = out[:, 128 * x : 128 * x + 128]
    send[...] = lines[...].reshape(8, 32, 128).astype(BF16)


def mix_kernel(received, forward, inverse, weights_ref, send, modes, mixed, weights=None, arrived=None):
    def weight_copy(g):
        return pltpu.make_async_copy(weights_ref.at[:, :, g], weights.at[:, :, g], arrived.at[g])

    if weights is None:
        weights = weights_ref
    else:
        for g in range(8):
            weight_copy(g).start()
    own = received.shape[2]
    data = received[...].astype(F32)
    data = jnp.concatenate([data[:, m].reshape(8 * own, 128) for m in range(4)], axis=1)
    out = dot(forward[...], data.astype(BF16))
    out = out[:KEPT] + turn(out[KEPT:])
    out = jnp.concatenate([out[:, 128 * m : 128 * m + 128] for m in range(4)], axis=0)
    modes[...] = out.T

    def step(g, sums):
        if arrived is not None:
            weight_copy(g).wait()
        sums = list(sums)
        base = g * 16
        for h in range(4):
            for k in range(2):
                real = modes[pl.ds(base + 4 * k + h, 1), :]
                imag = modes[pl.ds(base + 8 + 4 * k + h, 1), :]
                w_real = weights[0, h, g, k].astype(F32)
                w_imag = weights[1, h, g, k].astype(F32)
                sums[2 * k] = sums[2 * k] + (w_real * real - w_imag * imag)
                sums[2 * k + 1] = sums[2 * k + 1] + (w_real * imag + w_imag * real)
        return tuple(sums)

    sums = lax.fori_loop(0, 8, step, tuple(jnp.zeros((C, 128), F32) for _ in range(4)))
    for k in range(2):
        for r in range(2):
            for h in range(4):
                mixed[pl.ds(8 * r + 4 * k + h, 8, stride=16), :] = sums[2 * k + r][8 * h : 8 * h + 8]
    back = mixed[...].T
    back = jnp.concatenate([back[32 * m : 32 * m + 32] for m in range(4)], axis=1)
    back = jnp.concatenate([back, turn(back)], axis=0).astype(BF16)
    out = dot(inverse[...], jnp.concatenate([back, back], axis=0))
    for m in range(4):
        send[:, m] = out[:, 128 * m : 128 * m + 128].reshape(8, own, 128).astype(BF16)


def back_columns(lines, table, own, first, count):
    data = jnp.concatenate([lines[pl.ds(first + x, KEPT, stride=own), :] for x in range(count)], axis=1)
    data = jnp.concatenate([data, turn(data)], axis=0).astype(BF16)
    return dot(table, jnp.concatenate([data, data], axis=0))


def back_fine_kernel(received, table, send, lines):
    lines[...] = received[...].astype(F32).reshape(512, 128)
    for pair in range(8):
        out = back_columns(lines, table[...], 16, 2 * pair, 2)
        parts = [out[:, 128 * e : 128 * e + 128].reshape(16, 1, 8, 128) for e in range(2)]
        block = jnp.concatenate(parts, axis=1).reshape(16, 16, 128)
        send[:, 16 * pair : 16 * pair + 16, :] = block.astype(BF16)


def back_coarse_kernel(received, table, send, lines, cells):
    lines[...] = received[...].astype(F32).reshape(256, 128)
    out = back_columns(lines, table[...], 8, 0, 8)
    for x in range(8):
        cells[pl.ds(x, 64, stride=8), :] = out[:, 128 * x : 128 * x + 128]
    send[...] = cells[...].reshape(16, 32, 128).astype(BF16)


def channel_map(mixing):
    row = lax.broadcasted_iota(jnp.int32, (512, C), 0)
    channel = lax.broadcasted_iota(jnp.int32, (512, C), 1)
    pick = jnp.where((row >> 4) == channel, 1.0, 0.0).astype(BF16)
    wide = lax.dot_general(pick, mixing, (((1,), (1,)), ((), ())), preferred_element_type=F32)
    wide = lax.dot_general(wide.astype(BF16), pick, (((1,), (1,)), ((), ())), preferred_element_type=F32)
    a = lax.broadcasted_iota(jnp.int32, (512, 512), 0)
    b = lax.broadcasted_iota(jnp.int32, (512, 512), 1)
    return jnp.where(((a ^ b) & 15) == 0, wide, 0.0).astype(BF16)


def pointwise_kernel(field, mix_fine, bias, mix_coarse, total, map_coarse):
    channels = channel_map(mix_fine[...])
    for pair in range(4):
        rows = [slice(32 * pair + 16 * e, 32 * pair + 16 * e + 16) for e in range(2)]
        out = dot(channels, jnp.concatenate([field[:, at, :].reshape(512, 128) for at in rows], axis=1))
        for o in range(C):
            for e in range(2):
                total[o, rows[e], :] = out[16 * o : 16 * o + 16, 128 * e : 128 * e + 128] + bias[o]
    map_coarse[...] = channel_map(mix_coarse[...])


def gelu(v):
    inner = v * (0.7978845608028654 + 0.03567740813636141 * (v * v))
    half = 0.5 * v
    return half + half * jnp.tanh(inner)


def upper_kernel(received, table, total, next_table, upper, pooled, send, spread, sums, product):
    collect_groups(received, spread, 128)
    even = (lanes_of((64, 128)) & 1) == 0
    for g in range(8):
        out = dot(spread[g], table[...])
        for h in range(4):
            o = 8 * h + g
            value = gelu(out[:, 128 * h : 128 * h + 128] + total[o]).astype(BF16)
            upper[o] = value
            value = value.astype(F32).reshape(8, 2, 8, 128)
            value = (value[:, 0] + value[:, 1]).reshape(64, 128)
            sums[o] = value + jnp.where(even, pltpu.roll(value, 127, 1), pltpu.roll(value, 1, 1))
    for o in range(C):
        parts = [sums[o, pl.ds(2 * y, 8, stride=8), :] + sums[o, pl.ds(2 * y + 1, 8, stride=8), :] for y in range(4)]
        pooled[o] = (jnp.concatenate(parts, axis=0) * 0.125).astype(BF16)
    for g in range(8):
        rows = jnp.concatenate([pooled[8 * h + g] for h in range(4)], axis=1)
        product[g] = dot(rows, next_table[...])
    spread_groups(product, send, 32)


def lower_kernel(received, table, pooled, channels, bias, upper, out_ref, spread, total, sums, merged, left):
    blocks = [pooled[:, 16 * p : 16 * p + 16, :].reshape(512, 128) for p in range(2)]
    own = dot(channels[...], jnp.concatenate(blocks, axis=1))
    for p in range(2):
        total[:, 16 * p : 16 * p + 16, :] = own[:, 128 * p : 128 * p + 128].reshape(C, 16, 128)
    collect_groups(received, spread, 32)
    copies = [pltpu.make_async_copy(merged.at[g], out_ref.at[:, g], left.at[g]) for g in range(8)]
    for g in range(8):
        out = dot(spread[g], table[...])
        for h in range(4):
            o = 8 * h + g
            value = gelu(out[:, 128 * h : 128 * h + 128] + total[o] + bias[o]).astype(BF16).astype(F32)
            for y in range(4):
                part = value[8 * y : 8 * y + 8]
                sums[o, pl.ds(2 * y, 8, stride=8), :] = part
                sums[o, pl.ds(2 * y + 1, 8, stride=8), :] = part
            added = sums[o].reshape(8, 1, 8, 128)
            fine = upper[o].astype(F32).reshape(8, 2, 8, 128)
            merged[g, h] = (fine + added).reshape(128, 128).astype(BF16)
        copies[g].start()
    for copy in copies:
        copy.wait()


VMEM = pl.BlockSpec(memory_space=pltpu.VMEM)
SMEM = pl.BlockSpec(memory_space=pltpu.SMEM)
HBM = pl.BlockSpec(memory_space=pltpu.HBM)


def call(kernel, outs, *operands, scratch=(), specs=None, out_specs=None, limit=8):
    shapes = [jax.ShapeDtypeStruct(shape, kind) for shape, kind in outs]
    out_specs = out_specs or [VMEM] * len(shapes)
    return pl.pallas_call(
        kernel,
        out_shape=shapes if len(shapes) > 1 else shapes[0],
        in_specs=specs or [VMEM] * len(operands),
        out_specs=out_specs if len(shapes) > 1 else out_specs[0],
        scratch_shapes=[pltpu.VMEM(*s) if isinstance(s, tuple) else s for s in scratch],
        compiler_params=pltpu.CompilerParams(vmem_limit_bytes=limit << 20),
    )(*operands)


hold = pltpu.with_memory_space_constraint


def exchange(x, axis):
    return lax.all_to_all(x, axis, 0, 0, tiled=True)


def lay_out(spectral):
    place = jnp.asarray(np.eye(128).reshape(4, 32, 128).astype(BF16))
    return jnp.einsum("riojmk,mjl->rikol", spectral, place, preferred_element_type=BF16)


def on_device(field, spec_fine, mix_fine, bias_fine, spec_coarse, mix_coarse, bias_coarse):
    field = field.reshape(C, 128, 128)
    forward_fine, inverse_fine = jnp.asarray(plane_forward(128)), jnp.asarray(plane_inverse(128))
    forward_coarse, inverse_coarse = jnp.asarray(plane_forward(64)), jnp.asarray(plane_inverse(64))

    x = call(
        depth_kernel,
        [((16, 128, 128), BF16)],
        hold(field.reshape(4, 8, 128, 128), pltpu.HBM),
        hold(jnp.asarray(depth_forward(128, 1)), pltpu.HBM),
        specs=[HBM, HBM],
        out_specs=[HBM],
        scratch=[
            ((8, 4, 128, 128), BF16),
            ((512, 256), BF16),
            ((8, 128, 256), F32),
            ((16, 128, 128), BF16),
            pltpu.SemaphoreType.DMA((9,)),
            pltpu.SemaphoreType.DMA((8,)),
        ],
    )
    x = exchange(x, "py")
    weights_fine = lay_out(spec_fine)
    spec_coarse, weights_fine = lax.optimization_barrier((spec_coarse, weights_fine))
    weights_coarse = lay_out(spec_coarse)
    field, weights_coarse = lax.optimization_barrier((field, weights_coarse))
    total, map_coarse = call(
        pointwise_kernel,
        [((C, 128, 128), F32), ((512, 512), BF16)],
        field,
        mix_fine,
        bias_fine,
        mix_coarse,
        specs=[VMEM, VMEM, SMEM, VMEM],
    )
    x, weights_fine, weights_coarse, total, map_coarse = lax.optimization_barrier(
        (x, weights_fine, weights_coarse, total, map_coarse)
    )
    weights_fine = hold(weights_fine.reshape(2, 4, 8, 2, C, 128), pltpu.HBM)
    weights_coarse = weights_coarse.reshape(2, 4, 8, 2, C, 128)
    x = call(columns_fine_kernel, [((8, 64, 128), BF16)], x, forward_fine, scratch=[((512, 128), F32)])
    x = exchange(x, "px").reshape(8, 4, 16, 128)
    mix_scratch = [((128, 128), F32), ((128, 128), F32)]
    own_weights = [((2, 4, 8, 2, C, 128), BF16), pltpu.SemaphoreType.DMA((8,))]
    x = call(mix_kernel, [((8, 4, 16, 128), BF16)], x, forward_fine, inverse_fine, weights_fine, specs=[VMEM, VMEM, VMEM, HBM], scratch=mix_scratch + own_weights)
    x = exchange(x.reshape(8, 64, 128), "px")
    x = call(back_fine_kernel, [((16, 128, 128), BF16)], x, inverse_fine, scratch=[((512, 128), F32)])
    x = exchange(x, "py")
    upper, pooled, x = call(
        upper_kernel,
        [((C, 128, 128), BF16), ((C, 32, 128), BF16), ((16, 32, 128), BF16)],
        x,
        jnp.asarray(depth_inverse(128, 1)),
        total,
        jnp.asarray(depth_forward(64, 2)),
        scratch=[((8, 128, 256), BF16), ((C, 64, 128), F32), ((8, 32, 256), F32)],
        limit=12,
    )
    x = exchange(x, "py")
    scratch = [((512, 128), F32), ((256, 128), F32)]
    x = call(columns_coarse_kernel, [((8, 32, 128), BF16)], x, forward_coarse, scratch=scratch)
    x = exchange(x, "px").reshape(8, 4, 8, 128)
    x = call(mix_kernel, [((8, 4, 8, 128), BF16)], x, forward_coarse, inverse_coarse, weights_coarse, scratch=mix_scratch)
    x = exchange(x.reshape(8, 32, 128), "px")
    x = call(back_coarse_kernel, [((16, 32, 128), BF16)], x, inverse_coarse, scratch=scratch[::-1])
    x = exchange(x, "py")
    out = call(
        lower_kernel,
        [((4, 8, 128, 128), BF16)],
        x,
        jnp.asarray(depth_inverse(64, 2)),
        pooled,
        map_coarse,
        bias_coarse,
        upper,
        specs=[VMEM, VMEM, VMEM, VMEM, SMEM, VMEM],
        out_specs=[HBM],
        scratch=[
            ((8, 32, 256), BF16),
            ((C, 32, 128), F32),
            ((C, 64, 128), F32),
            ((8, 4, 128, 128), BF16),
            pltpu.SemaphoreType.DMA((8,)),
        ],
        limit=12,
    )
    return out.reshape(C, 16, 8, 128)


def solution(mesh):
    return jax.shard_map(
        on_device,
        mesh=mesh,
        in_specs=(
            P(None, "px", "py", None),
            P(None, None, None, None, "px", "py"),
            P(),
            P(),
            P(None, None, None, None, "px", "py"),
            P(),
            P(),
        ),
        out_specs=P(None, "px", "py", None),
        check_vma=False,
    )
```

```python
import functools
import math

import jax
import jax.numpy as jnp
import numpy as np
from jax import lax
from jax.experimental import pallas as pl
from jax.experimental.pallas import tpu as pltpu
from jax.sharding import PartitionSpec as P

C = 32
KEPT = 32
F32 = jnp.float32
BF16 = jnp.bfloat16


def angles(cells, offset):
    windings = np.arange(cells)[:, None] * (np.arange(KEPT)[None, :] - offset) % cells
    return windings.astype(np.float64) * (2.0 * math.pi / cells)


def depth_forward(cells, repeat):
    angle = angles(cells, 0)
    table = np.stack([np.cos(angle), -np.sin(angle)])
    table = table.reshape(2, cells, 16, 2).transpose(1, 2, 0, 3)
    spread = np.zeros((cells, repeat) + table.shape[1:])
    spread[:, 0] = table
    spread = spread.reshape((cells * repeat,) + table.shape[1:])
    result = np.einsum("zprk,hg->hzprkg", spread, np.eye(4))
    return result.reshape(4 * cells * repeat, 256).astype(BF16)


def plane_forward(cells):
    angle = angles(cells, KEPT // 2)
    return np.concatenate([np.cos(angle), -np.sin(angle)], axis=1).T.astype(BF16)


def halves(table):
    high = table.astype(np.float32).astype(BF16)
    low = (table.astype(np.float32) - high.astype(np.float32)).astype(BF16)
    return high, low


def plane_inverse(cells):
    angle = angles(cells, KEPT // 2)
    high, low = halves(np.concatenate([np.cos(angle), np.sin(angle)], axis=1))
    return np.concatenate([high, low], axis=1)


def depth_inverse(cells, repeat):
    angle = angles(cells, 0)
    factor = np.where(np.arange(KEPT) == 0, 1.0, 2.0) / float(cells**3)
    table = np.stack([factor * np.cos(angle), -factor * np.sin(angle)])
    table = np.repeat(table, repeat, axis=1).reshape(2, cells * repeat, 16, 2)
    result = np.einsum("rzpk,hg->prkhgz", table, np.eye(4)).reshape(256, 4 * cells * repeat)
    return result.astype(BF16)


def dot(a, b):
    return jnp.dot(a, b, preferred_element_type=F32)


def lanes_of(shape):
    return lax.broadcasted_iota(jnp.int32, shape, len(shape) - 1)


def turn(x):
    width = x.shape[-1]
    real = (lanes_of(x.shape) & 8) == 0
    return jnp.where(real, -pltpu.roll(x, width - 8, 1), pltpu.roll(x, 8, 1))


def swap_blocks(parts):
    parts = list(parts)
    lane = lanes_of(parts[0].shape)
    for step in (1, 2, 4):
        keep = (lane & (16 * step)) == 0
        for low in range(8):
            if low & step == 0:
                a, b = parts[low], parts[low + step]
                parts[low] = jnp.where(keep, a, pltpu.roll(b, 16 * step, 1))
                parts[low + step] = jnp.where(keep, pltpu.roll(a, 128 - 16 * step, 1), b)
    return parts


def spread_groups(product, send, rows, sent=None):
    def chunk(index, carry):
        at = pl.ds(pl.multiple_of(index * 16, 16), 16)
        for half in range(2):
            parts = swap_blocks([product[g, at, 128 * half : 128 * half + 128] for g in range(8)])
            for b in range(8):
                send[8 * half + b, at, :] = parts[b].astype(BF16)
        if sent is not None:
            sent(index, at)
        return carry

    lax.fori_loop(0, rows // 16, chunk, 0, unroll=min(2, rows // 16))


def collect_groups(received, spread, rows):
    def chunk(index, carry):
        at = pl.ds(pl.multiple_of(index * 16, 16), 16)
        for half in range(2):
            parts = swap_blocks([received[8 * half + b, at, :].astype(F32) for b in range(8)])
            for g in range(8):
                spread[g, at, 128 * half : 128 * half + 128] = parts[g].astype(BF16)
        return carry

    lax.fori_loop(0, rows // 16, chunk, 0, unroll=min(2, rows // 16))


def depth_kernel(field, table_ref, send_ref, values, table, product, send, arrived, left):
    copies = [pltpu.make_async_copy(field.at[:, g], values.at[g], arrived.at[g]) for g in range(8)]
    table_copy = pltpu.make_async_copy(table_ref, table, arrived.at[8])
    copies[0].start()
    table_copy.start()
    for copy in copies[1:]:
        copy.start()
    table_copy.wait()

    def group(pair, carry):
        for e in range(2):
            g = 2 * pair + e
            pltpu.make_async_copy(field.at[:, g], values.at[g], arrived.at[g]).wait()
        for e in range(2):
            rows = jnp.concatenate([values[2 * pair + e, h] for h in range(4)], axis=1)
            product[2 * pair + e] = dot(rows, table[...])
        return carry

    lax.fori_loop(0, 4, group, 0)

    def leave(index, at):
        pltpu.make_async_copy(send.at[:, at, :], send_ref.at[:, at, :], left.at[index]).start()

    spread_groups(product, send, 128, leave)
    for index in range(8):
        at = pl.ds(16 * index, 16)
        pltpu.make_async_copy(send.at[:, at, :], send_ref.at[:, at, :], left.at[index]).wait()


def columns_fine_kernel(received, table, later, send, lines):
    del later
    for pair in range(8):
        block = received[:, 16 * pair : 16 * pair + 16, :].astype(F32).reshape(16, 2, 8, 128)
        data = jnp.concatenate([block[:, e].reshape(128, 128) for e in range(2)], axis=1)
        out = dot(table[...], data.astype(BF16))
        out = out[:KEPT] + turn(out[KEPT:])
        for e in range(2):
            lines[pl.ds(2 * pair + e, KEPT, stride=16), :] = out[:, 128 * e : 128 * e + 128]
    send[...] = lines[...].reshape(8, 64, 128).astype(BF16)


def columns_coarse_kernel(received, table, send, cells, lines):
    cells[...] = received[...].astype(F32).reshape(512, 128)
    data = jnp.concatenate([cells[pl.ds(x, 64, stride=8), :] for x in range(8)], axis=1)
    out = dot(table[...], data.astype(BF16))
    out = out[:KEPT] + turn(out[KEPT:])
    for x in range(8):
        lines[pl.ds(x, KEPT, stride=8), :] = out[:, 128 * x : 128 * x + 128]
    send[...] = lines[...].reshape(8, 32, 128).astype(BF16)


def mix_kernel(received, forward, inverse, weights_ref, send, modes, mixed, weights=None, arrived=None):
    def weight_copy(g):
        return pltpu.make_async_copy(weights_ref.at[:, :, g], weights.at[:, :, g], arrived.at[g])

    if weights is None:
        weights = weights_ref
    else:
        for g in range(8):
            weight_copy(g).start()
    own = received.shape[2]
    data = received[...].astype(F32)
    data = jnp.concatenate([data[:, m].reshape(8 * own, 128) for m in range(4)], axis=1)
    out = dot(forward[...], data.astype(BF16))
    out = out[:KEPT] + turn(out[KEPT:])
    out = jnp.concatenate([out[:, 128 * m : 128 * m + 128] for m in range(4)], axis=0)
    modes[...] = out.T

    def step(g, sums):
        if arrived is not None:
            weight_copy(g).wait()
        sums = list(sums)
        base = g * 16
        for h in range(4):
            for k in range(2):
                real = modes[pl.ds(base + 4 * k + h, 1), :]
                imag = modes[pl.ds(base + 8 + 4 * k + h, 1), :]
                w_real = weights[0, h, g, k].astype(F32)
                w_imag = weights[1, h, g, k].astype(F32)
                sums[2 * k] = sums[2 * k] + (w_real * real - w_imag * imag)
                sums[2 * k + 1] = sums[2 * k + 1] + (w_real * imag + w_imag * real)
        return tuple(sums)

    sums = lax.fori_loop(0, 8, step, tuple(jnp.zeros((C, 128), F32) for _ in range(4)))
    for k in range(2):
        for r in range(2):
            for h in range(4):
                mixed[pl.ds(8 * r + 4 * k + h, 8, stride=16), :] = sums[2 * k + r][8 * h : 8 * h + 8]
    back = mixed[...].T
    back = jnp.concatenate([back[32 * m : 32 * m + 32] for m in range(4)], axis=1)
    back = jnp.concatenate([back, turn(back)], axis=0).astype(BF16)
    out = dot(inverse[...], jnp.concatenate([back, back], axis=0))
    for m in range(4):
        send[:, m] = out[:, 128 * m : 128 * m + 128].reshape(8, own, 128).astype(BF16)


def back_columns(lines, table, own, first, count):
    data = jnp.concatenate([lines[pl.ds(first + x, KEPT, stride=own), :] for x in range(count)], axis=1)
    data = jnp.concatenate([data, turn(data)], axis=0).astype(BF16)
    return dot(table, jnp.concatenate([data, data], axis=0))


def back_fine_kernel(received, table, send, lines):
    lines[...] = received[...].astype(F32).reshape(512, 128)
    for pair in range(8):
        out = back_columns(lines, table[...], 16, 2 * pair, 2)
        parts = [out[:, 128 * e : 128 * e + 128].reshape(16, 1, 8, 128) for e in range(2)]
        block = jnp.concatenate(parts, axis=1).reshape(16, 16, 128)
        send[:, 16 * pair : 16 * pair + 16, :] = block.astype(BF16)


def back_coarse_kernel(received, table, send, lines, cells):
    lines[...] = received[...].astype(F32).reshape(256, 128)
    out = back_columns(lines, table[...], 8, 0, 8)
    for x in range(8):
        cells[pl.ds(x, 64, stride=8), :] = out[:, 128 * x : 128 * x + 128]
    send[...] = cells[...].reshape(16, 32, 128).astype(BF16)


def channel_map(mixing):
    row = lax.broadcasted_iota(jnp.int32, (512, C), 0)
    channel = lax.broadcasted_iota(jnp.int32, (512, C), 1)
    pick = jnp.where((row >> 4) == channel, 1.0, 0.0).astype(BF16)
    wide = lax.dot_general(pick, mixing, (((1,), (1,)), ((), ())), preferred_element_type=F32)
    wide = lax.dot_general(wide.astype(BF16), pick, (((1,), (1,)), ((), ())), preferred_element_type=F32)
    a = lax.broadcasted_iota(jnp.int32, (512, 512), 0)
    b = lax.broadcasted_iota(jnp.int32, (512, 512), 1)
    return jnp.where(((a ^ b) & 15) == 0, wide, 0.0).astype(BF16)


def pointwise_kernel(field, mix_fine, bias, mix_coarse, total, map_coarse):
    channels = channel_map(mix_fine[...])
    for pair in range(4):
        rows = [slice(32 * pair + 16 * e, 32 * pair + 16 * e + 16) for e in range(2)]
        out = dot(channels, jnp.concatenate([field[:, at, :].reshape(512, 128) for at in rows], axis=1))
        for o in range(C):
            for e in range(2):
                block = out[16 * o : 16 * o + 16, 128 * e : 128 * e + 128] + bias[o]
                total[o, rows[e], :] = block.astype(BF16)
    map_coarse[...] = channel_map(mix_coarse[...])


def gelu(v):
    inner = v * (0.7978845608028654 + 0.03567740813636141 * (v * v))
    half = 0.5 * v
    return half + half * jnp.tanh(inner)


def upper_kernel(received, table, total, next_table, upper, pooled, send, spread, sums, product):
    collect_groups(received, spread, 128)
    even = (lanes_of((64, 128)) & 1) == 0
    for g in range(8):
        for h in range(4):
            if h % 2 == 0:
                out = dot(spread[g], table[:, 128 * h : 128 * h + 256])
            o = 8 * h + g
            value = gelu(out[:, 128 * (h % 2) : 128 * (h % 2) + 128] + total[o].astype(F32)).astype(BF16)
            upper[o] = value
            value = value.astype(F32).reshape(8, 2, 8, 128)
            value = (value[:, 0] + value[:, 1]).reshape(64, 128)
            sums[o] = value + jnp.where(even, pltpu.roll(value, 127, 1), pltpu.roll(value, 1, 1))
    for o in range(C):
        parts = [sums[o, pl.ds(2 * y, 8, stride=8), :] + sums[o, pl.ds(2 * y + 1, 8, stride=8), :] for y in range(4)]
        pooled[o] = (jnp.concatenate(parts, axis=0) * 0.125).astype(BF16)
    for g in range(8):
        rows = jnp.concatenate([pooled[8 * h + g] for h in range(4)], axis=1)
        product[g] = dot(rows, next_table[...])
    spread_groups(product, send, 32)


def lower_kernel(received, table, pooled, channels, bias, upper, out_ref, spread, total, sums, merged, left):
    blocks = [pooled[:, 16 * p : 16 * p + 16, :].reshape(512, 128) for p in range(2)]
    own = dot(channels[...], jnp.concatenate(blocks, axis=1))
    for p in range(2):
        total[:, 16 * p : 16 * p + 16, :] = own[:, 128 * p : 128 * p + 128].reshape(C, 16, 128)
    collect_groups(received, spread, 32)
    copies = [pltpu.make_async_copy(merged.at[g], out_ref.at[:, g], left.at[g]) for g in range(8)]
    for g in range(8):
        out = dot(spread[g], table[...])
        for h in range(4):
            o = 8 * h + g
            value = gelu(out[:, 128 * h : 128 * h + 128] + total[o] + bias[o]).astype(BF16).astype(F32)
            for y in range(4):
                part = value[8 * y : 8 * y + 8]
                sums[o, pl.ds(2 * y, 8, stride=8), :] = part
                sums[o, pl.ds(2 * y + 1, 8, stride=8), :] = part
            added = sums[o].reshape(8, 1, 8, 128)
            fine = upper[o].astype(F32).reshape(8, 2, 8, 128)
            merged[g, h] = (fine + added).reshape(128, 128).astype(BF16)
        copies[g].start()
    for copy in copies:
        copy.wait()


VMEM = pl.BlockSpec(memory_space=pltpu.VMEM)
SMEM = pl.BlockSpec(memory_space=pltpu.SMEM)
HBM = pl.BlockSpec(memory_space=pltpu.HBM)


def call(kernel, outs, *operands, scratch=(), specs=None, out_specs=None, limit=8):
    shapes = [jax.ShapeDtypeStruct(shape, kind) for shape, kind in outs]
    out_specs = out_specs or [VMEM] * len(shapes)
    return pl.pallas_call(
        kernel,
        out_shape=shapes if len(shapes) > 1 else shapes[0],
        in_specs=specs or [VMEM] * len(operands),
        out_specs=out_specs if len(shapes) > 1 else out_specs[0],
        scratch_shapes=[pltpu.VMEM(*s) if isinstance(s, tuple) else s for s in scratch],
        compiler_params=pltpu.CompilerParams(vmem_limit_bytes=limit << 20),
    )(*operands)


hold = pltpu.with_memory_space_constraint


def exchange(x, axis):
    return lax.all_to_all(x, axis, 0, 0, tiled=True)


def lay_out(spectral):
    place = jnp.asarray(np.eye(128).reshape(4, 32, 128).astype(BF16))
    return jnp.einsum("riojmk,mjl->rikol", spectral, place, preferred_element_type=BF16)


def on_device(field, spec_fine, mix_fine, bias_fine, spec_coarse, mix_coarse, bias_coarse):
    field = field.reshape(C, 128, 128)
    forward_fine, inverse_fine = jnp.asarray(plane_forward(128)), jnp.asarray(plane_inverse(128))
    forward_coarse, inverse_coarse = jnp.asarray(plane_forward(64)), jnp.asarray(plane_inverse(64))

    x = call(
        depth_kernel,
        [((16, 128, 128), BF16)],
        hold(field.reshape(4, 8, 128, 128), pltpu.HBM),
        hold(jnp.asarray(depth_forward(128, 1)), pltpu.HBM),
        specs=[HBM, HBM],
        out_specs=[HBM],
        scratch=[
            ((8, 4, 128, 128), BF16),
            ((512, 256), BF16),
            ((8, 128, 256), F32),
            ((16, 128, 128), BF16),
            pltpu.SemaphoreType.DMA((9,)),
            pltpu.SemaphoreType.DMA((8,)),
        ],
    )
    x = exchange(x, "py")
    weights_fine = lay_out(spec_fine)
    spec_coarse, weights_fine = lax.optimization_barrier((spec_coarse, weights_fine))
    weights_coarse = lay_out(spec_coarse)
    field, weights_coarse = lax.optimization_barrier((field, weights_coarse))
    total, map_coarse = call(
        pointwise_kernel,
        [((C, 128, 128), BF16), ((512, 512), BF16)],
        field,
        mix_fine,
        bias_fine,
        mix_coarse,
        specs=[VMEM, VMEM, SMEM, VMEM],
    )
    x, weights_fine, weights_coarse, total, map_coarse = lax.optimization_barrier(
        (x, weights_fine, weights_coarse, total, map_coarse)
    )
    weights_fine = weights_fine.reshape(2, 4, 8, 2, C, 128)
    weights_coarse = weights_coarse.reshape(2, 4, 8, 2, C, 128)
    x = call(columns_fine_kernel, [((8, 64, 128), BF16)], x, forward_fine, weights_fine, scratch=[((512, 128), F32)])
    x = exchange(x, "px").reshape(8, 4, 16, 128)
    mix_scratch = [((128, 128), F32), ((128, 128), F32)]
    own_weights = [((2, 4, 8, 2, C, 128), BF16), pltpu.SemaphoreType.DMA((8,))]
    x = call(mix_kernel, [((8, 4, 16, 128), BF16)], x, forward_fine, inverse_fine, weights_fine, scratch=mix_scratch)
    x = exchange(x.reshape(8, 64, 128), "px")
    x = call(back_fine_kernel, [((16, 128, 128), BF16)], x, inverse_fine, scratch=[((512, 128), F32)])
    x = exchange(x, "py")
    upper, pooled, x = call(
        upper_kernel,
        [((C, 128, 128), BF16), ((C, 32, 128), BF16), ((16, 32, 128), BF16)],
        x,
        jnp.asarray(depth_inverse(128, 1)),
        total,
        jnp.asarray(depth_forward(64, 2)),
        scratch=[((8, 128, 256), BF16), ((C, 64, 128), F32), ((8, 32, 256), F32)],
        limit=12,
    )
    x = exchange(x, "py")
    scratch = [((512, 128), F32), ((256, 128), F32)]
    x = call(columns_coarse_kernel, [((8, 32, 128), BF16)], x, forward_coarse, scratch=scratch)
    x = exchange(x, "px").reshape(8, 4, 8, 128)
    x = call(mix_kernel, [((8, 4, 8, 128), BF16)], x, forward_coarse, inverse_coarse, weights_coarse, scratch=mix_scratch)
    x = exchange(x.reshape(8, 32, 128), "px")
    x = call(back_coarse_kernel, [((16, 32, 128), BF16)], x, inverse_coarse, scratch=scratch[::-1])
    x = exchange(x, "py")
    out = call(
        lower_kernel,
        [((4, 8, 128, 128), BF16)],
        x,
        jnp.asarray(depth_inverse(64, 2)),
        pooled,
        map_coarse,
        bias_coarse,
        upper,
        specs=[VMEM, VMEM, VMEM, VMEM, SMEM, VMEM],
        out_specs=[HBM],
        scratch=[
            ((8, 32, 256), BF16),
            ((C, 32, 128), F32),
            ((C, 64, 128), F32),
            ((8, 4, 128, 128), BF16),
            pltpu.SemaphoreType.DMA((8,)),
        ],
        limit=12,
    )
    return out.reshape(C, 16, 8, 128)


def solution(mesh):
    return jax.shard_map(
        on_device,
        mesh=mesh,
        in_specs=(
            P(None, "px", "py", None),
            P(None, None, None, None, "px", "py"),
            P(),
            P(),
            P(None, None, None, None, "px", "py"),
            P(),
            P(),
        ),
        out_specs=P(None, "px", "py", None),
        check_vma=False,
    )
```

```python
import functools
import math

import jax
import jax.numpy as jnp
import numpy as np
from jax import lax
from jax.experimental import pallas as pl
from jax.experimental.pallas import tpu as pltpu
from jax.sharding import PartitionSpec as P

C = 32
KEPT = 32
F32 = jnp.float32
BF16 = jnp.bfloat16


def angles(cells, offset):
    windings = np.arange(cells)[:, None] * (np.arange(KEPT)[None, :] - offset) % cells
    return windings.astype(np.float64) * (2.0 * math.pi / cells)


def depth_forward(cells, repeat):
    angle = angles(cells, 0)
    table = np.stack([np.cos(angle), -np.sin(angle)])
    table = table.reshape(2, cells, 16, 2).transpose(1, 2, 0, 3)
    spread = np.zeros((cells, repeat) + table.shape[1:])
    spread[:, 0] = table
    spread = spread.reshape((cells * repeat,) + table.shape[1:])
    result = np.einsum("zprk,hg->hzprkg", spread, np.eye(4))
    return result.reshape(4 * cells * repeat, 256).astype(BF16)


def plane_forward(cells):
    angle = angles(cells, KEPT // 2)
    return np.concatenate([np.cos(angle), -np.sin(angle)], axis=1).T.astype(BF16)


def halves(table):
    high = table.astype(np.float32).astype(BF16)
    low = (table.astype(np.float32) - high.astype(np.float32)).astype(BF16)
    return high, low


def plane_inverse(cells):
    angle = angles(cells, KEPT // 2)
    high, low = halves(np.concatenate([np.cos(angle), np.sin(angle)], axis=1))
    return np.concatenate([high, low], axis=1)


def depth_inverse(cells, repeat):
    angle = angles(cells, 0)
    factor = np.where(np.arange(KEPT) == 0, 1.0, 2.0) / float(cells**3)
    table = np.stack([factor * np.cos(angle), -factor * np.sin(angle)])
    table = np.repeat(table, repeat, axis=1).reshape(2, cells * repeat, 16, 2)
    result = np.einsum("rzpk,hg->prkhgz", table, np.eye(4)).reshape(256, 4 * cells * repeat)
    return result.astype(BF16)


def dot(a, b):
    return jnp.dot(a, b, preferred_element_type=F32)


def lanes_of(shape):
    return lax.broadcasted_iota(jnp.int32, shape, len(shape) - 1)


def turn(x):
    width = x.shape[-1]
    real = (lanes_of(x.shape) & 8) == 0
    return jnp.where(real, -pltpu.roll(x, width - 8, 1), pltpu.roll(x, 8, 1))


def swap_blocks(parts):
    parts = list(parts)
    lane = lanes_of(parts[0].shape)
    for step in (1, 2, 4):
        keep = (lane & (16 * step)) == 0
        for low in range(8):
            if low & step == 0:
                a, b = parts[low], parts[low + step]
                parts[low] = jnp.where(keep, a, pltpu.roll(b, 16 * step, 1))
                parts[low + step] = jnp.where(keep, pltpu.roll(a, 128 - 16 * step, 1), b)
    return parts


def spread_groups(product, send, rows, sent=None):
    def chunk(index, carry):
        at = pl.ds(pl.multiple_of(index * 16, 16), 16)
        for half in range(2):
            parts = swap_blocks([product[g, at, 128 * half : 128 * half + 128] for g in range(8)])
            for b in range(8):
                send[8 * half + b, at, :] = parts[b].astype(BF16)
        if sent is not None:
            sent(index, at)
        return carry

    lax.fori_loop(0, rows // 16, chunk, 0, unroll=min(2, rows // 16))


def collect_groups(received, spread, rows):
    def chunk(index, carry):
        at = pl.ds(pl.multiple_of(index * 16, 16), 16)
        for half in range(2):
            parts = swap_blocks([received[8 * half + b, at, :].astype(F32) for b in range(8)])
            for g in range(8):
                spread[g, at, 128 * half : 128 * half + 128] = parts[g].astype(BF16)
        return carry

    lax.fori_loop(0, rows // 16, chunk, 0, unroll=min(2, rows // 16))


def depth_kernel(field, table_ref, send_ref, values, table, product, send, arrived, left):
    copies = [pltpu.make_async_copy(field.at[:, g], values.at[g], arrived.at[g]) for g in range(8)]
    table_copy = pltpu.make_async_copy(table_ref, table, arrived.at[8])
    copies[0].start()
    table_copy.start()
    for copy in copies[1:]:
        copy.start()
    table_copy.wait()

    def group(pair, carry):
        for e in range(2):
            g = 2 * pair + e
            pltpu.make_async_copy(field.at[:, g], values.at[g], arrived.at[g]).wait()
        for e in range(2):
            rows = jnp.concatenate([values[2 * pair + e, h] for h in range(4)], axis=1)
            product[2 * pair + e] = dot(rows, table[...])
        return carry

    lax.fori_loop(0, 4, group, 0)

    def leave(index, at):
        pltpu.make_async_copy(send.at[:, at, :], send_ref.at[:, at, :], left.at[index]).start()

    spread_groups(product, send, 128, leave)
    for index in range(8):
        at = pl.ds(16 * index, 16)
        pltpu.make_async_copy(send.at[:, at, :], send_ref.at[:, at, :], left.at[index]).wait()


def columns_fine_kernel(received, table, later, send, lines):
    del later
    for pair in range(8):
        block = received[:, 16 * pair : 16 * pair + 16, :].astype(F32).reshape(16, 2, 8, 128)
        data = jnp.concatenate([block[:, e].reshape(128, 128) for e in range(2)], axis=1)
        out = dot(table[...], data.astype(BF16))
        out = out[:KEPT] + turn(out[KEPT:])
        for e in range(2):
            lines[pl.ds(2 * pair + e, KEPT, stride=16), :] = out[:, 128 * e : 128 * e + 128]
    send[...] = lines[...].reshape(8, 64, 128).astype(BF16)


def columns_coarse_kernel(received, table, send, cells, lines):
    cells[...] = received[...].astype(F32).reshape(512, 128)
    data = jnp.concatenate([cells[pl.ds(x, 64, stride=8), :] for x in range(8)], axis=1)
    out = dot(table[...], data.astype(BF16))
    out = out[:KEPT] + turn(out[KEPT:])
    for x in range(8):
        lines[pl.ds(x, KEPT, stride=8), :] = out[:, 128 * x : 128 * x + 128]
    send[...] = lines[...].reshape(8, 32, 128).astype(BF16)


def mix_kernel(received, forward, inverse, weights_ref, send, modes, mixed, weights=None, arrived=None):
    def weight_copy(g):
        return pltpu.make_async_copy(weights_ref.at[:, :, g], weights.at[:, :, g], arrived.at[g])

    if weights is None:
        weights = weights_ref
    else:
        for g in range(8):
            weight_copy(g).start()
    own = received.shape[2]
    data = received[...].astype(F32)
    data = jnp.concatenate([data[:, m].reshape(8 * own, 128) for m in range(4)], axis=1)
    out = dot(forward[...], data.astype(BF16))
    out = out[:KEPT] + turn(out[KEPT:])
    out = jnp.concatenate([out[:, 128 * m : 128 * m + 128] for m in range(4)], axis=0)
    modes[...] = out.T

    def step(g, sums):
        if arrived is not None:
            weight_copy(g).wait()
        sums = list(sums)
        base = g * 16
        for h in range(4):
            for k in range(2):
                real = modes[pl.ds(base + 4 * k + h, 1), :]
                imag = modes[pl.ds(base + 8 + 4 * k + h, 1), :]
                w_real = weights[0, h, g, k].astype(F32)
                w_imag = weights[1, h, g, k].astype(F32)
                sums[2 * k] = sums[2 * k] + (w_real * real - w_imag * imag)
                sums[2 * k + 1] = sums[2 * k + 1] + (w_real * imag + w_imag * real)
        return tuple(sums)

    sums = lax.fori_loop(0, 8, step, tuple(jnp.zeros((C, 128), F32) for _ in range(4)), unroll=4)
    for k in range(2):
        for r in range(2):
            for h in range(4):
                mixed[pl.ds(8 * r + 4 * k + h, 8, stride=16), :] = sums[2 * k + r][8 * h : 8 * h + 8]
    back = mixed[...].T
    back = jnp.concatenate([back[32 * m : 32 * m + 32] for m in range(4)], axis=1)
    back = jnp.concatenate([back, turn(back)], axis=0).astype(BF16)
    out = dot(inverse[...], jnp.concatenate([back, back], axis=0))
    for m in range(4):
        send[:, m] = out[:, 128 * m : 128 * m + 128].reshape(8, own, 128).astype(BF16)


def back_columns(lines, table, own, first, count):
    data = jnp.concatenate([lines[pl.ds(first + x, KEPT, stride=own), :] for x in range(count)], axis=1)
    data = jnp.concatenate([data, turn(data)], axis=0).astype(BF16)
    return dot(table, jnp.concatenate([data, data], axis=0))


def back_fine_kernel(received, table, send, lines):
    lines[...] = received[...].astype(F32).reshape(512, 128)
    for pair in range(8):
        out = back_columns(lines, table[...], 16, 2 * pair, 2)
        parts = [out[:, 128 * e : 128 * e + 128].reshape(16, 1, 8, 128) for e in range(2)]
        block = jnp.concatenate(parts, axis=1).reshape(16, 16, 128)
        send[:, 16 * pair : 16 * pair + 16, :] = block.astype(BF16)


def back_coarse_kernel(received, table, send, lines, cells):
    lines[...] = received[...].astype(F32).reshape(256, 128)
    out = back_columns(lines, table[...], 8, 0, 8)
    for x in range(8):
        cells[pl.ds(x, 64, stride=8), :] = out[:, 128 * x : 128 * x + 128]
    send[...] = cells[...].reshape(16, 32, 128).astype(BF16)


def channel_map(mixing):
    row = lax.broadcasted_iota(jnp.int32, (512, C), 0)
    channel = lax.broadcasted_iota(jnp.int32, (512, C), 1)
    pick = jnp.where((row >> 4) == channel, 1.0, 0.0).astype(BF16)
    wide = lax.dot_general(pick, mixing, (((1,), (1,)), ((), ())), preferred_element_type=F32)
    wide = lax.dot_general(wide.astype(BF16), pick, (((1,), (1,)), ((), ())), preferred_element_type=F32)
    a = lax.broadcasted_iota(jnp.int32, (512, 512), 0)
    b = lax.broadcasted_iota(jnp.int32, (512, 512), 1)
    return jnp.where(((a ^ b) & 15) == 0, wide, 0.0).astype(BF16)


def pointwise_kernel(field, mix_fine, bias, mix_coarse, total, map_coarse):
    channels = channel_map(mix_fine[...])
    for pair in range(4):
        rows = [slice(32 * pair + 16 * e, 32 * pair + 16 * e + 16) for e in range(2)]
        out = dot(channels, jnp.concatenate([field[:, at, :].reshape(512, 128) for at in rows], axis=1))
        for o in range(C):
            for e in range(2):
                block = out[16 * o : 16 * o + 16, 128 * e : 128 * e + 128] + bias[o]
                total[o, rows[e], :] = block.astype(BF16)
    map_coarse[...] = channel_map(mix_coarse[...])


def gelu(v):
    inner = v * (0.7978845608028654 + 0.03567740813636141 * (v * v))
    half = 0.5 * v
    return half + half * jnp.tanh(inner)


def upper_kernel(received, table, total, next_table, upper, pooled, send, spread, sums, product):
    collect_groups(received, spread, 128)
    even = (lanes_of((64, 128)) & 1) == 0
    for g in range(8):
        out = dot(spread[g], table[...])
        for h in range(4):
            o = 8 * h + g
            value = gelu(out[:, 128 * h : 128 * h + 128] + total[o].astype(F32)).astype(BF16)
            upper[o] = value
            value = value.astype(F32).reshape(8, 2, 8, 128)
            value = (value[:, 0] + value[:, 1]).reshape(64, 128)
            sums[o] = value + jnp.where(even, pltpu.roll(value, 127, 1), pltpu.roll(value, 1, 1))
    for o in range(C):
        parts = [sums[o, pl.ds(2 * y, 8, stride=8), :] + sums[o, pl.ds(2 * y + 1, 8, stride=8), :] for y in range(4)]
        pooled[o] = (jnp.concatenate(parts, axis=0) * 0.125).astype(BF16)
    for g in range(8):
        rows = jnp.concatenate([pooled[8 * h + g] for h in range(4)], axis=1)
        product[g] = dot(rows, next_table[...])
    spread_groups(product, send, 32)


def lower_kernel(received, table, pooled, channels, bias, upper, out_ref, spread, total, sums, merged, left):
    blocks = [pooled[:, 16 * p : 16 * p + 16, :].reshape(512, 128) for p in range(2)]
    own = dot(channels[...], jnp.concatenate(blocks, axis=1))
    for p in range(2):
        total[:, 16 * p : 16 * p + 16, :] = own[:, 128 * p : 128 * p + 128].reshape(C, 16, 128)
    collect_groups(received, spread, 32)
    copies = [pltpu.make_async_copy(merged.at[g], out_ref.at[:, g], left.at[g]) for g in range(8)]
    for g in range(8):
        out = dot(spread[g], table[...])
        for h in range(4):
            o = 8 * h + g
            value = gelu(out[:, 128 * h : 128 * h + 128] + total[o] + bias[o]).astype(BF16).astype(F32)
            for y in range(4):
                part = value[8 * y : 8 * y + 8]
                sums[o, pl.ds(2 * y, 8, stride=8), :] = part
                sums[o, pl.ds(2 * y + 1, 8, stride=8), :] = part
            added = sums[o].reshape(8, 1, 8, 128)
            fine = upper[o].astype(F32).reshape(8, 2, 8, 128)
            merged[g, h] = (fine + added).reshape(128, 128).astype(BF16)
        copies[g].start()
    for copy in copies:
        copy.wait()


VMEM = pl.BlockSpec(memory_space=pltpu.VMEM)
SMEM = pl.BlockSpec(memory_space=pltpu.SMEM)
HBM = pl.BlockSpec(memory_space=pltpu.HBM)


def call(kernel, outs, *operands, scratch=(), specs=None, out_specs=None, limit=8):
    shapes = [jax.ShapeDtypeStruct(shape, kind) for shape, kind in outs]
    out_specs = out_specs or [VMEM] * len(shapes)
    return pl.pallas_call(
        kernel,
        out_shape=shapes if len(shapes) > 1 else shapes[0],
        in_specs=specs or [VMEM] * len(operands),
        out_specs=out_specs if len(shapes) > 1 else out_specs[0],
        scratch_shapes=[pltpu.VMEM(*s) if isinstance(s, tuple) else s for s in scratch],
        compiler_params=pltpu.CompilerParams(vmem_limit_bytes=limit << 20),
    )(*operands)


hold = pltpu.with_memory_space_constraint


def exchange(x, axis):
    return lax.all_to_all(x, axis, 0, 0, tiled=True)


def lay_out(spectral):
    place = jnp.asarray(np.eye(128).reshape(4, 32, 128).astype(BF16))
    return jnp.einsum("riojmk,mjl->rikol", spectral, place, preferred_element_type=BF16)


def on_device(field, spec_fine, mix_fine, bias_fine, spec_coarse, mix_coarse, bias_coarse):
    field = field.reshape(C, 128, 128)
    forward_fine, inverse_fine = jnp.asarray(plane_forward(128)), jnp.asarray(plane_inverse(128))
    forward_coarse, inverse_coarse = jnp.asarray(plane_forward(64)), jnp.asarray(plane_inverse(64))

    x = call(
        depth_kernel,
        [((16, 128, 128), BF16)],
        hold(field.reshape(4, 8, 128, 128), pltpu.HBM),
        hold(jnp.asarray(depth_forward(128, 1)), pltpu.HBM),
        specs=[HBM, HBM],
        out_specs=[HBM],
        scratch=[
            ((8, 4, 128, 128), BF16),
            ((512, 256), BF16),
            ((8, 128, 256), F32),
            ((16, 128, 128), BF16),
            pltpu.SemaphoreType.DMA((9,)),
            pltpu.SemaphoreType.DMA((8,)),
        ],
    )
    x = exchange(x, "py")
    weights_fine = lay_out(spec_fine)
    spec_coarse, weights_fine = lax.optimization_barrier((spec_coarse, weights_fine))
    weights_coarse = lay_out(spec_coarse)
    field, weights_coarse = lax.optimization_barrier((field, weights_coarse))
    total, map_coarse = call(
        pointwise_kernel,
        [((C, 128, 128), BF16), ((512, 512), BF16)],
        field,
        mix_fine,
        bias_fine,
        mix_coarse,
        specs=[VMEM, VMEM, SMEM, VMEM],
    )
    x, weights_fine, weights_coarse, total, map_coarse = lax.optimization_barrier(
        (x, weights_fine, weights_coarse, total, map_coarse)
    )
    weights_fine = weights_fine.reshape(2, 4, 8, 2, C, 128)
    weights_coarse = weights_coarse.reshape(2, 4, 8, 2, C, 128)
    x = call(columns_fine_kernel, [((8, 64, 128), BF16)], x, forward_fine, weights_fine, scratch=[((512, 128), F32)])
    x = exchange(x, "px").reshape(8, 4, 16, 128)
    mix_scratch = [((128, 128), F32), ((128, 128), F32)]
    own_weights = [((2, 4, 8, 2, C, 128), BF16), pltpu.SemaphoreType.DMA((8,))]
    x = call(mix_kernel, [((8, 4, 16, 128), BF16)], x, forward_fine, inverse_fine, weights_fine, scratch=mix_scratch)
    x = exchange(x.reshape(8, 64, 128), "px")
    x = call(back_fine_kernel, [((16, 128, 128), BF16)], x, inverse_fine, scratch=[((512, 128), F32)])
    x = exchange(x, "py")
    upper, pooled, x = call(
        upper_kernel,
        [((C, 128, 128), BF16), ((C, 32, 128), BF16), ((16, 32, 128), BF16)],
        x,
        jnp.asarray(depth_inverse(128, 1)),
        total,
        jnp.asarray(depth_forward(64, 2)),
        scratch=[((8, 128, 256), BF16), ((C, 64, 128), F32), ((8, 32, 256), F32)],
        limit=12,
    )
    x = exchange(x, "py")
    scratch = [((512, 128), F32), ((256, 128), F32)]
    x = call(columns_coarse_kernel, [((8, 32, 128), BF16)], x, forward_coarse, scratch=scratch)
    x = exchange(x, "px").reshape(8, 4, 8, 128)
    x = call(mix_kernel, [((8, 4, 8, 128), BF16)], x, forward_coarse, inverse_coarse, weights_coarse, scratch=mix_scratch)
    x = exchange(x.reshape(8, 32, 128), "px")
    x = call(back_coarse_kernel, [((16, 32, 128), BF16)], x, inverse_coarse, scratch=scratch[::-1])
    x = exchange(x, "py")
    out = call(
        lower_kernel,
        [((4, 8, 128, 128), BF16)],
        x,
        jnp.asarray(depth_inverse(64, 2)),
        pooled,
        map_coarse,
        bias_coarse,
        upper,
        specs=[VMEM, VMEM, VMEM, VMEM, SMEM, VMEM],
        out_specs=[HBM],
        scratch=[
            ((8, 32, 256), BF16),
            ((C, 32, 128), F32),
            ((C, 64, 128), F32),
            ((8, 4, 128, 128), BF16),
            pltpu.SemaphoreType.DMA((8,)),
        ],
        limit=12,
    )
    return out.reshape(C, 16, 8, 128)


def solution(mesh):
    return jax.shard_map(
        on_device,
        mesh=mesh,
        in_specs=(
            P(None, "px", "py", None),
            P(None, None, None, None, "px", "py"),
            P(),
            P(),
            P(None, None, None, None, "px", "py"),
            P(),
            P(),
        ),
        out_specs=P(None, "px", "py", None),
        check_vma=False,
    )
```
